32 devices in a mesh: pair: 1 (over z), tp: 4 (over y), side: 8 (over x, core).
Axes of the slice: x: 4, y: 4, z: 1, core: 2. Of those that a mesh axis runs over, the one named last changes fastest.
The devices are a block of a 4x4x8 slice.
Arguments:
- x: bfloat16 [2048, 2048], P(('pair', 'side'))
- req_len: int32 [8], P('pair')
- dest: int32 [8], P('pair')
- w_qkv: bfloat16 [2, 2048, 3072], replicated
- w_out: bfloat16 [2, 2048, 2048], replicated
- w_gate: bfloat16 [2, 2048, 8192], replicated
- w_up: bfloat16 [2, 2048, 8192], replicated
- w_down: bfloat16 [2, 8192, 2048], replicated
- y_tok: bfloat16 [8, 64, 2048], P(('pair', 'side'))
- k_cache: bfloat16 [8, 2, 64, 128, 8, 64], P(('pair', 'side'), None, None, None, 'tp')
- v_cache: bfloat16 [8, 2, 64, 128, 8, 64], P(('pair', 'side'), None, None, None, 'tp')
- c_len: int32 [8, 64], P(('pair', 'side'))
Outputs:
- output 1: bfloat16 [2048, 2048], P(('pair', 'side'))
- output 2: bfloat16 [8, 64, 2048], P(('pair', 'side'))
- output 3: bfloat16 [8, 2, 448, 8, 64], P(('pair', 'side'), None, None, 'tp')
- output 4: bfloat16 [8, 2, 448, 8, 64], P(('pair', 'side'), None, None, 'tp')
- output 5: bfloat16 [8, 2, 64, 128, 8, 64], P(('pair', 'side'), None, None, None, 'tp')
- output 6: bfloat16 [8, 2, 64, 128, 8, 64], P(('pair', 'side'), None, None, None, 'tp')
All inputs are finite; a program needn't handle non-finite values.
Results may differ from the reference program's by a relative error of at most 0.0173637.
Values are sent between devices in bfloat16 or wider.
A program may use at most 768 MiB of HBM per device.

```python
import jax
import jax.numpy as jnp
from jax import lax

TP_SIZE = 4
SIDE_SIZE = 8
MODEL_DIM = 2048
HEADS = 32
KV_HEADS = 8
HEAD_DIM = 64
FF_DIM = 8192
LAYERS = 2
PROMPT_ROWS = 256
BATCH = 64
CACHE_LEN = 128
SEQ_LEN = PROMPT_ROWS * SIDE_SIZE
MAX_REQ = 2 * PROMPT_ROWS - PROMPT_ROWS // 4
GROUP_REP = HEADS // KV_HEADS
KV_LOCAL = KV_HEADS // TP_SIZE
Q_COLS = HEADS * HEAD_DIM
KV_COLS = KV_HEADS * HEAD_DIM
ROPE_BASE = 10000.0
NORM_EPS = 1e-5


def draw_normal(key, shape, scale):
    return (jax.random.normal(key, shape, jnp.float32) * scale).astype(jnp.bfloat16)


def draw_lengths(key):
    quarter = PROMPT_ROWS // 4
    eighth = PROMPT_ROWS // 8
    key_first, key_gap = jax.random.split(key)
    first_len = jax.random.randint(key_first, (SIDE_SIZE // 2,), quarter, 2 * PROMPT_ROWS - quarter + 1)
    gap_len = jax.random.randint(key_gap, (SIDE_SIZE // 2,), 0, eighth + 1)
    first_len = first_len.at[0].set(MAX_REQ)
    gap_len = gap_len.at[0].set(eighth)
    second_len = 2 * PROMPT_ROWS - gap_len - first_len
    return jnp.stack([first_len, second_len], axis=1).reshape(SIDE_SIZE).astype(jnp.int32)


def draw_cache_lengths(key):
    lengths = jax.random.randint(key, (SIDE_SIZE, BATCH), CACHE_LEN // 2, CACHE_LEN)
    lengths = lengths.at[:, 0].set(CACHE_LEN - 1)
    lengths = lengths.at[:, 1].set(CACHE_LEN // 2)
    return lengths.astype(jnp.int32)


def setup_inputs(seed: int = 0, part: int = 0) -> dict:
    part_keys = jax.random.split(jax.random.fold_in(jax.random.key(seed), part), 7)
    weight_keys = jax.random.split(jax.random.key(seed + 1), 5)
    cache_shape = (SIDE_SIZE, LAYERS, BATCH, CACHE_LEN, KV_HEADS, HEAD_DIM)
    return {
        'x': draw_normal(part_keys[0], (SEQ_LEN, MODEL_DIM), 1.0),
        'req_len': draw_lengths(part_keys[1]),
        'dest': jax.random.permutation(part_keys[2], SIDE_SIZE).astype(jnp.int32),
        'w_qkv': draw_normal(weight_keys[0], (LAYERS, MODEL_DIM, Q_COLS + 2 * KV_COLS), MODEL_DIM ** -0.5),
        'w_out': draw_normal(weight_keys[1], (LAYERS, Q_COLS, MODEL_DIM), Q_COLS ** -0.5),
        'w_gate': draw_normal(weight_keys[2], (LAYERS, MODEL_DIM, FF_DIM), MODEL_DIM ** -0.5),
        'w_up': draw_normal(weight_keys[3], (LAYERS, MODEL_DIM, FF_DIM), MODEL_DIM ** -0.5),
        'w_down': draw_normal(weight_keys[4], (LAYERS, FF_DIM, MODEL_DIM), FF_DIM ** -0.5),
        'y_tok': draw_normal(part_keys[3], (SIDE_SIZE, BATCH, MODEL_DIM), 1.0),
        'k_cache': draw_normal(part_keys[4], cache_shape, 1.0),
        'v_cache': draw_normal(part_keys[5], cache_shape, 1.0),
        'c_len': draw_cache_lengths(part_keys[6]),
    }


def rms_norm(hidden):
    wide_vals = hidden.astype(jnp.float32)
    norm_scale = lax.rsqrt(jnp.mean(wide_vals * wide_vals, axis=-1, keepdims=True) + NORM_EPS)
    return (wide_vals * norm_scale).astype(jnp.bfloat16)


def rotary(vectors, positions):
    half_dim = HEAD_DIM // 2
    inv_freq = ROPE_BASE ** (-jnp.arange(half_dim, dtype=jnp.float32) / half_dim)
    angles = positions.astype(jnp.float32)[:, None, None] * inv_freq
    cos_val = jnp.cos(angles)
    sin_val = jnp.sin(angles)
    wide_vals = vectors.astype(jnp.float32)
    lead_half = wide_vals[..., :half_dim]
    tail_half = wide_vals[..., half_dim:]
    return jnp.concatenate([lead_half * cos_val - tail_half * sin_val, tail_half * cos_val + lead_half * sin_val], axis=-1).astype(jnp.bfloat16)


def b_order(array_in, axis):
    shape_in = array_in.shape
    split_shape = shape_in[:axis] + (KV_LOCAL, TP_SIZE) + shape_in[axis + 1:]
    return jnp.swapaxes(array_in.reshape(split_shape), axis, axis + 1).reshape(shape_in)


def split_qkv(w_qkv):
    return w_qkv[..., :Q_COLS], w_qkv[..., Q_COLS:Q_COLS + KV_COLS], w_qkv[..., Q_COLS + KV_COLS:]


def project(hidden, wq_l, wk_l, wv_l, positions):
    row_count = hidden.shape[0]
    normed = rms_norm(hidden)
    query = jnp.dot(normed, wq_l, preferred_element_type=jnp.float32).astype(jnp.bfloat16)
    key_new = jnp.dot(normed, wk_l, preferred_element_type=jnp.float32).astype(jnp.bfloat16)
    value_new = jnp.dot(normed, wv_l, preferred_element_type=jnp.float32).astype(jnp.bfloat16)
    query = rotary(query.reshape(row_count, HEADS, HEAD_DIM), positions)
    key_new = rotary(key_new.reshape(row_count, KV_HEADS, HEAD_DIM), positions)
    return query.reshape(row_count, KV_HEADS, GROUP_REP, HEAD_DIM), key_new, value_new.reshape(row_count, KV_HEADS, HEAD_DIM)


def finish_layer(hidden, context, wo_l, wg_l, wu_l, wd_l):
    attn_out = jnp.dot(context, wo_l, preferred_element_type=jnp.float32).astype(jnp.bfloat16)
    hidden = (hidden.astype(jnp.float32) + attn_out.astype(jnp.float32)).astype(jnp.bfloat16)
    normed = rms_norm(hidden)
    gate = jnp.dot(normed, wg_l, preferred_element_type=jnp.float32).astype(jnp.bfloat16)
    upper = jnp.dot(normed, wu_l, preferred_element_type=jnp.float32).astype(jnp.bfloat16)
    activated = (jax.nn.silu(gate.astype(jnp.float32)) * upper.astype(jnp.float32)).astype(jnp.bfloat16)
    down = jnp.dot(activated, wd_l, preferred_element_type=jnp.float32).astype(jnp.bfloat16)
    return (hidden.astype(jnp.float32) + down.astype(jnp.float32)).astype(jnp.bfloat16)


def prefill(x, req_len, w_qkv, w_out, w_gate, w_up, w_down):
    row_ids = jnp.arange(SEQ_LEN)
    past_end = row_ids[:, None] >= jnp.cumsum(req_len)[None, :]
    seg_id = jnp.sum(past_end.astype(jnp.int32), axis=1)
    positions = row_ids - jnp.sum(jnp.where(past_end, req_len[None, :], 0), axis=1)
    allowed = (seg_id[:, None] == seg_id[None, :]) & (row_ids[None, :] <= row_ids[:, None])
    w_q, w_k, w_v = split_qkv(w_qkv)

    def head_attention(operands):
        q_head, k_head, v_head = operands
        scores = jnp.einsum('srd,td->rst', q_head.astype(jnp.float32), k_head.astype(jnp.float32)) * HEAD_DIM ** -0.5
        scores = jnp.where(allowed[None], scores, -1e30)
        attn_prob = jax.nn.softmax(scores, axis=-1).astype(jnp.bfloat16)
        return jnp.einsum('rst,td->srd', attn_prob.astype(jnp.float32), v_head.astype(jnp.float32)).astype(jnp.bfloat16)

    def layer_step(hidden, weights):
        wq_l, wk_l, wv_l, wo_l, wg_l, wu_l, wd_l = weights
        query, key_new, value_new = project(hidden, wq_l, wk_l, wv_l, positions)
        context = lax.map(head_attention, (jnp.swapaxes(query, 0, 1), jnp.swapaxes(key_new, 0, 1), jnp.swapaxes(value_new, 0, 1)))
        context = jnp.swapaxes(context, 0, 1).reshape(SEQ_LEN, Q_COLS)
        return finish_layer(hidden, context, wo_l, wg_l, wu_l, wd_l), (key_new, value_new)

    return lax.scan(layer_step, x, (w_q, w_k, w_v, w_out, w_gate, w_up, w_down))


def install(full, req_len, dest):
    starts = jnp.cumsum(req_len) - req_len
    match = dest[None, :] == jnp.arange(SIDE_SIZE)[:, None]
    start_of = jnp.sum(jnp.where(match, starts[None, :], 0), axis=1)
    length_of = jnp.sum(jnp.where(match, req_len[None, :], 0), axis=1)
    padded = jnp.concatenate([full, jnp.zeros((LAYERS, MAX_REQ, KV_HEADS, HEAD_DIM), full.dtype)], axis=1)

    def one_group(start_row, length):
        piece = lax.dynamic_slice_in_dim(padded, start_row, MAX_REQ, axis=1)
        keep = (jnp.arange(MAX_REQ) < length)[None, :, None, None]
        return b_order(jnp.where(keep, piece, jnp.zeros_like(piece)), 2)

    return jax.vmap(one_group)(start_of, length_of)


def decode(y_tok, k_cache, v_cache, c_len, w_qkv, w_out, w_gate, w_up, w_down):
    w_q, w_k, w_v = split_qkv(w_qkv)
    wq_b = b_order(w_q.reshape(LAYERS, MODEL_DIM, KV_HEADS, GROUP_REP * HEAD_DIM), 2).reshape(LAYERS, MODEL_DIM, Q_COLS)
    wk_b = b_order(w_k.reshape(LAYERS, MODEL_DIM, KV_HEADS, HEAD_DIM), 2).reshape(LAYERS, MODEL_DIM, KV_COLS)
    wv_b = b_order(w_v.reshape(LAYERS, MODEL_DIM, KV_HEADS, HEAD_DIM), 2).reshape(LAYERS, MODEL_DIM, KV_COLS)
    wo_b = b_order(w_out.reshape(LAYERS, KV_HEADS, GROUP_REP * HEAD_DIM, MODEL_DIM), 1).reshape(LAYERS, Q_COLS, MODEL_DIM)
    cache_pos = jnp.arange(CACHE_LEN)

    def one_group(operands):
        tokens, k_group, v_group, lengths = operands
        visible = cache_pos[None, :] <= lengths[:, None]
        at_slot = (cache_pos[None, :] == lengths[:, None])[:, :, None, None]

        def layer_step(hidden, weights):
            wq_l, wk_l, wv_l, wo_l, wg_l, wu_l, wd_l, k_layer, v_layer = weights
            query, key_new, value_new = project(hidden, wq_l, wk_l, wv_l, lengths)
            k_layer = jnp.where(at_slot, key_new[:, None], k_layer)
            v_layer = jnp.where(at_slot, value_new[:, None], v_layer)
            scores = jnp.einsum('bkrd,btkd->bkrt', query.astype(jnp.float32), k_layer.astype(jnp.float32)) * HEAD_DIM ** -0.5
            scores = jnp.where(visible[:, None, None, :], scores, -1e30)
            attn_prob = jax.nn.softmax(scores, axis=-1).astype(jnp.bfloat16)
            context = jnp.einsum('bkrt,btkd->bkrd', attn_prob.astype(jnp.float32), v_layer.astype(jnp.float32)).astype(jnp.bfloat16)
            hidden = finish_layer(hidden, context.reshape(BATCH, Q_COLS), wo_l, wg_l, wu_l, wd_l)
            return hidden, (k_layer, v_layer)

        hidden, (k_new, v_new) = lax.scan(layer_step, tokens, (wq_b, wk_b, wv_b, wo_b, w_gate, w_up, w_down, k_group, v_group))
        return hidden, k_new, v_new

    return lax.map(one_group, (y_tok, k_cache, v_cache, c_len))


def reference(x, req_len, dest, w_qkv, w_out, w_gate, w_up, w_down, y_tok, k_cache, v_cache, c_len):
    hidden, (keys_all, values_all) = prefill(x, req_len, w_qkv, w_out, w_gate, w_up, w_down)
    k_prompt = install(keys_all, req_len, dest)
    v_prompt = install(values_all, req_len, dest)
    dec_out, k_new, v_new = decode(y_tok, k_cache, v_cache, c_len, w_qkv, w_out, w_gate, w_up, w_down)
    return (hidden, dec_out, k_prompt, v_prompt, k_new, v_new)
```

```python
import functools

import jax
import jax.numpy as jnp
from jax import lax
from jax.experimental import pallas as pl
from jax.experimental.pallas import tpu as pltpu
from jax.sharding import PartitionSpec as P

ROPE_BASE = 10000.0
NORM_EPS = 1e-5
BF16 = jnp.bfloat16
F32 = jnp.float32
TILE = 512
W_SLOTS = 10
D_SLOTS = 4
ANY = pl.BlockSpec(memory_space=pl.ANY)
VMEM = pl.BlockSpec(memory_space=pltpu.VMEM)
SMEM = pl.BlockSpec(memory_space=pltpu.SMEM)
NT = (((1,), (1,)), ((), ()))


def rms(wide):
    return (wide * lax.rsqrt(jnp.mean(wide * wide, axis=-1, keepdims=True) + NORM_EPS)).astype(BF16)


def rope_tile(vals, cos, sin):
    wide = vals.astype(F32)
    width = wide.shape[1]
    lane = lax.broadcasted_iota(jnp.int32, wide.shape, 1)
    half = 32
    other = jnp.where(lax.rem(lane, 2 * half) < half, pltpu.roll(wide, width - half, 1), pltpu.roll(wide, half, 1))
    reps = width // cos.shape[1]
    return (wide * jnp.concatenate([cos] * reps, axis=1) + other * jnp.concatenate([sin] * reps, axis=1)).astype(BF16)


def trunk_kernel(layer, has_mid, has_qkv, *refs):
    refs = list(refs)
    h_ref = refs.pop(0)
    if has_mid:
        ctx_ref, wo_ref, wg_ref, wu_ref, wd_ref = refs[:5]
        refs = refs[5:]
    if has_qkv:
        cos_ref, sin_ref, wq_ref = refs[:3]
        refs = refs[3:]
    if has_mid:
        hout_ref = refs.pop(0)
    if has_qkv:
        qkv_ref = refs.pop(0)
    wbuf, wsem, dbuf, dsem, norm_ref, mid_ref, acc_ref = refs

    model = h_ref.shape[1]
    n_out = model // TILE if has_mid else 0
    n_ff = wg_ref.shape[2] // TILE if has_mid else 0
    n_qkv = wq_ref.shape[2] // TILE if has_qkv else 0
    qkv_layer = layer + 1 if has_mid else layer
    first_qkv = n_out + 2 * n_ff
    total = first_qkv + n_qkv

    def cols(src, lay, tile):
        return src.at[lay, :, pl.ds(pl.multiple_of(tile * TILE, TILE), TILE)]

    def w_start(src, lay, tile, slot):
        pltpu.make_async_copy(cols(src, lay, tile), wbuf.at[slot], wsem.at[slot]).start()

    def w_start_static(idx):
        slot = idx % W_SLOTS
        if idx < n_out:
            w_start(wo_ref, layer, idx, slot)
        elif idx < first_qkv:
            w_start((wg_ref, wu_ref)[(idx - n_out) % 2], layer, (idx - n_out) // 2, slot)
        elif idx < total:
            w_start(wq_ref, qkv_layer, idx - first_qkv, slot)

    def w_wait(slot):
        src = wq_ref if has_qkv else wo_ref
        pltpu.make_async_copy(cols(src, 0, 0), wbuf.at[slot], wsem.at[slot]).wait()

    def d_copy(chunk, slot):
        return pltpu.make_async_copy(wd_ref.at[layer, pl.ds(pl.multiple_of(chunk * TILE, TILE), TILE), :], dbuf.at[slot], dsem.at[slot])

    for idx in range(min(W_SLOTS, total)):
        w_start_static(idx)
        if has_mid and n_out <= idx < n_out + D_SLOTS:
            d_copy(idx - n_out, idx - n_out).start()

    if has_mid:
        for tile in range(n_out):
            slot = tile % W_SLOTS
            w_wait(slot)
            sl = slice(tile * TILE, (tile + 1) * TILE)
            out = jnp.dot(ctx_ref[...], wbuf[slot], preferred_element_type=F32).astype(BF16)
            w_start_static(tile + W_SLOTS)
            mid_ref[:, sl] = h_ref[:, sl].astype(F32) + out.astype(F32)
        hidden = mid_ref[...].astype(BF16)
        mid_ref[...] = hidden.astype(F32)
        norm_ref[...] = rms(mid_ref[...])
        acc_ref[...] = jnp.zeros_like(acc_ref)

        def chunk_step(chunk, carry):
            base = n_out + 2 * chunk
            slot_g = lax.rem(base, W_SLOTS)
            slot_u = lax.rem(base + 1, W_SLOTS)
            slot_d = lax.rem(chunk, D_SLOTS)
            w_wait(slot_g)
            gate = jnp.dot(norm_ref[...], wbuf[slot_g], preferred_element_type=F32).astype(BF16).astype(F32)
            w_wait(slot_u)
            upper = jnp.dot(norm_ref[...], wbuf[slot_u], preferred_element_type=F32).astype(BF16).astype(F32)
            act = (jax.nn.silu(gate) * upper).astype(BF16)
            ahead = W_SLOTS // 2

            @pl.when(chunk + ahead < n_ff)
            def _():
                w_start(wg_ref, layer, chunk + ahead, slot_g)
                w_start(wu_ref, layer, chunk + ahead, slot_u)

            if has_qkv:
                later = 2 * (chunk + ahead - n_ff)

                @pl.when((chunk + ahead >= n_ff) & (later < n_qkv))
                def _():
                    w_start(wq_ref, qkv_layer, later, slot_g)
                    w_start(wq_ref, qkv_layer, later + 1, slot_u)

            d_copy(chunk, slot_d).wait()
            acc_ref[...] += jnp.dot(act, dbuf[slot_d], preferred_element_type=F32)

            @pl.when(chunk + D_SLOTS < n_ff)
            def _():
                d_copy(chunk + D_SLOTS, slot_d).start()

            return carry

        lax.fori_loop(0, n_ff, chunk_step, 0)
        hidden = (mid_ref[...] + acc_ref[...].astype(BF16).astype(F32)).astype(BF16)
        hout_ref[...] = hidden
    else:
        hidden = h_ref[...]
    if has_qkv:
        norm_ref[...] = rms(hidden.astype(F32))
        for tile in range(n_qkv):
            slot = (first_qkv + tile) % W_SLOTS
            w_wait(slot)
            sl = slice(tile * TILE, (tile + 1) * TILE)
            out = jnp.dot(norm_ref[...], wbuf[slot], preferred_element_type=F32).astype(BF16)
            if (first_qkv + tile + W_SLOTS) < total and not has_mid:
                w_start_static(first_qkv + tile + W_SLOTS)
            if tile < n_qkv - 1:
                out = rope_tile(out, cos_ref[...], sin_ref[...])
            qkv_ref[:, sl] = out


def trunk(layer, hidden, ctx, cos, sin, w_qkv, w_out, w_gate, w_up, w_down):
    rows, model = hidden.shape
    has_mid = ctx is not None
    has_qkv = cos is not None
    args, specs, outs = [hidden], [VMEM], []
    if has_mid:
        args += [ctx, w_out, w_gate, w_up, w_down]
        specs += [VMEM, ANY, ANY, ANY, ANY]
        outs.append(jax.ShapeDtypeStruct((rows, model), BF16))
    if has_qkv:
        args += [cos, sin, w_qkv]
        specs += [VMEM, VMEM, ANY]
        outs.append(jax.ShapeDtypeStruct((rows, w_qkv.shape[2]), BF16))
    return pl.pallas_call(
        functools.partial(trunk_kernel, layer, has_mid, has_qkv),
        out_shape=outs,
        in_specs=specs,
        out_specs=[VMEM] * len(outs),
        scratch_shapes=[
            pltpu.VMEM((W_SLOTS, model, TILE), BF16),
            pltpu.SemaphoreType.DMA((W_SLOTS,)),
            pltpu.VMEM((D_SLOTS, TILE, model), BF16),
            pltpu.SemaphoreType.DMA((D_SLOTS,)),
            pltpu.VMEM((rows, model), BF16),
            pltpu.VMEM((rows, model), F32),
            pltpu.VMEM((rows, model), F32),
        ],
        compiler_params=pltpu.CompilerParams(vmem_limit_bytes=48 * 2**20),
        name="trunk",
    )(*args)


def prompt_attn_kernel(head_dim, rep, start_ref, seg_ref, q_ref, kv_hbm, out_ref, kv_ref, sem):
    window = kv_ref.shape[0]
    kv_cols = kv_ref.shape[1] // 2
    rows = q_ref.shape[0]
    key0 = pl.multiple_of(start_ref[0], 16)
    copy = pltpu.make_async_copy(kv_hbm.at[pl.ds(key0, window), :], kv_ref, sem)
    copy.start()
    key_row = key0 + lax.broadcasted_iota(jnp.int32, (rows, window), 1)
    q_row = start_ref[1] + lax.broadcasted_iota(jnp.int32, (rows, window), 0)
    allowed = (key_row <= q_row) & (key_row >= seg_ref[...])
    scale = head_dim ** -0.5
    copy.wait()
    for head in range(kv_cols // head_dim):
        k_head = kv_ref[:, head * head_dim:(head + 1) * head_dim]
        v_head = kv_ref[:, kv_cols + head * head_dim:kv_cols + (head + 1) * head_dim]
        outs = []
        for sub in range(rep):
            at = (head * rep + sub) * head_dim
            scores = lax.dot_general(q_ref[:, at:at + head_dim], k_head, NT, preferred_element_type=F32) * scale
            scores = jnp.where(allowed, scores, -1e30)
            scores = jnp.exp(scores - jnp.max(scores, axis=-1, keepdims=True))
            prob = (scores * (1.0 / jnp.sum(scores, axis=-1, keepdims=True))).astype(BF16)
            outs.append(jnp.dot(prob, v_head, preferred_element_type=F32).astype(BF16))
        out_ref[:, head * rep * head_dim:(head + 1) * rep * head_dim] = jnp.concatenate(outs, axis=1)


def prompt_attn(query, kv_all, key0, row0, seg_start, window, head_dim, rep):
    rows = query.shape[0]
    return pl.pallas_call(
        functools.partial(prompt_attn_kernel, head_dim, rep),
        out_shape=jax.ShapeDtypeStruct(query.shape, BF16),
        in_specs=[SMEM, VMEM, VMEM, ANY],
        out_specs=VMEM,
        scratch_shapes=[pltpu.VMEM((window, kv_all.shape[1]), BF16), pltpu.SemaphoreType.DMA],
        compiler_params=pltpu.CompilerParams(vmem_limit_bytes=32 * 2**20),
        name="prompt_attn",
    )(jnp.stack([key0, row0]).astype(jnp.int32), seg_start, query, kv_all)


def decode_attn_kernel(head_dim, rep, pairs_per_b, len_ref, lenrow_ref, q_ref, kn_ref, vn_ref, k_ref, v_ref, *rest):
    ctx_ref, kout_ref, vout_ref = rest[-3:]
    step = pl.program_id(0)
    t_len = k_ref.shape[1]
    pairs = k_ref.shape[0] // head_dim
    group = 4
    batch = pairs // pairs_per_b
    t_iota = lax.broadcasted_iota(jnp.int32, (head_dim, t_len), 1)
    for pair in range(pairs):
        at = len_ref[step * batch + pair // pairs_per_b]
        here = t_iota == at
        sl = slice(pair * head_dim, (pair + 1) * head_dim)
        kout_ref[sl, :] = jnp.where(here, kn_ref[:, pair:pair + 1].astype(F32), k_ref[sl, :].astype(F32)).astype(BF16)
        vout_ref[sl, :] = jnp.where(here, vn_ref[:, pair:pair + 1].astype(F32), v_ref[sl, :].astype(F32)).astype(BF16)
    rows = group * rep
    width = group * head_dim
    diag = (lax.broadcasted_iota(jnp.int32, (rows, width), 0) // rep) == (lax.broadcasted_iota(jnp.int32, (rows, width), 1) // head_dim)
    scores = []
    for g in range(pairs // group):
        q_part = q_ref[g * rows:(g + 1) * rows, :].astype(F32)
        lhs = jnp.where(diag, jnp.concatenate([q_part] * group, axis=1), 0.0).astype(BF16)
        scores.append(jnp.dot(lhs, kout_ref[g * width:(g + 1) * width, :], preferred_element_type=F32))
    scores = jnp.concatenate(scores, axis=0) * (head_dim ** -0.5)
    t_row = lax.broadcasted_iota(jnp.int32, scores.shape, 1)
    scores = jnp.where(t_row <= lenrow_ref[...], scores, -1e30)
    scores = jnp.exp(scores - jnp.max(scores, axis=-1, keepdims=True))
    prob = (scores * (1.0 / jnp.sum(scores, axis=-1, keepdims=True))).astype(BF16)
    fold = (lax.rem(lax.broadcasted_iota(jnp.int32, (width, head_dim), 0), head_dim) == lax.broadcasted_iota(jnp.int32, (width, head_dim), 1)).astype(F32).astype(BF16)
    for g in range(pairs // group):
        full = lax.dot_general(prob[g * rows:(g + 1) * rows, :], vout_ref[g * width:(g + 1) * width, :], NT, preferred_element_type=F32)
        own = jnp.where(diag, full, 0.0).astype(BF16)
        ctx_ref[g * rows:(g + 1) * rows, :] = jnp.dot(own, fold, preferred_element_type=F32).astype(BF16)


def decode_attn(layer, query, k_cols, v_cols, lengths, kc, vc, prev, head_dim, rep, pairs_per_b, steps):
    layers, depth, t_len = kc.shape
    block = depth // steps
    q_rows = query.shape[0] // steps
    len_rows = jnp.repeat(lengths, pairs_per_b * rep)[:, None]
    cache_in = pl.BlockSpec((None, block, t_len), lambda i: (layer, i, 0))
    col_in = pl.BlockSpec((None, head_dim, k_cols.shape[2]), lambda i: (i, 0, 0))
    row_in = pl.BlockSpec((q_rows, head_dim), lambda i: (i, 0))
    args = [lengths, len_rows, query, k_cols, v_cols, kc, vc]
    specs = [SMEM, pl.BlockSpec((q_rows, 1), lambda i: (i, 0)), row_in, col_in, col_in, cache_in, cache_in]
    aliases = {}
    if prev is not None:
        args += list(prev)
        specs += [ANY, ANY]
        aliases = {7: 1, 8: 2}
    return pl.pallas_call(
        functools.partial(decode_attn_kernel, head_dim, rep, pairs_per_b),
        out_shape=[jax.ShapeDtypeStruct(query.shape, BF16), jax.ShapeDtypeStruct(kc.shape, BF16), jax.ShapeDtypeStruct(vc.shape, BF16)],
        grid=(steps,),
        in_specs=specs,
        out_specs=[row_in, cache_in, cache_in],
        input_output_aliases=aliases,
        compiler_params=pltpu.CompilerParams(vmem_limit_bytes=32 * 2**20),
        name="decode_attn",
    )(*args)


def solution(mesh):
    tp = mesh.shape['tp']
    side = mesh.shape['side']
    rows_spec = P(('pair', 'side'), None)
    batch_spec = P(('pair', 'side'), None, None)
    cache_spec = P(('pair', 'side'), None, None, None, 'tp', None)
    prompt_spec = P(('pair', 'side'), None, None, 'tp', None)

    def local_step(x_loc, req_len, dest, w_qkv, w_out, w_gate, w_up, w_down, y_loc, kc_loc, vc_loc, clen_loc):
        s_idx = lax.axis_index('side')
        t_idx = lax.axis_index('tp')
        layers = w_qkv.shape[0]
        head_dim = kc_loc.shape[-1]
        slots = kc_loc.shape[-2]
        t_len = kc_loc.shape[3]
        batch = y_loc.shape[1]
        kv_heads = slots * tp
        rep = w_out.shape[1] // head_dim // kv_heads
        q_cols = w_out.shape[1]
        kv_cols = kv_heads * head_dim
        prompt_rows = x_loc.shape[0]
        seq_len = prompt_rows * side
        max_req = 2 * prompt_rows - prompt_rows // 4
        p_rows = prompt_rows // tp
        d_rows = batch // tp

        hidden = jnp.concatenate([lax.dynamic_slice_in_dim(x_loc, t_idx * p_rows, p_rows, 0), lax.dynamic_slice_in_dim(y_loc[0], t_idx * d_rows, d_rows, 0)], axis=0)
        row0 = s_idx * prompt_rows + t_idx * p_rows
        ids = jnp.arange(side)
        ends = jnp.sum(jnp.where(ids[None, :] <= ids[:, None], req_len[None, :], 0), axis=1)
        row_ids = row0 + jnp.arange(p_rows)
        seg_start = jnp.sum(jnp.where(row_ids[:, None] >= ends[None, :], req_len[None, :], 0), axis=1)
        lengths = clen_loc[0]
        positions = jnp.concatenate([row_ids - seg_start, lax.dynamic_slice_in_dim(lengths, t_idx * d_rows, d_rows, 0)])
        half = head_dim // 2
        inv_freq = ROPE_BASE ** (-jnp.arange(half, dtype=F32) / half)
        angles = positions.astype(F32)[:, None] * inv_freq
        cos = jnp.cos(angles)
        sin = jnp.sin(angles)
        cos = jnp.concatenate([cos] * 4, axis=1)
        sin = jnp.concatenate([-sin, sin] * 2, axis=1)
        window = -(-(max_req - 1) // p_rows) * p_rows + p_rows
        key0 = jnp.maximum(row0 + p_rows - window, 0)

        kc = jnp.transpose(kc_loc[0], (0, 1, 3, 4, 2)).reshape(layers, batch * slots * head_dim, t_len)
        vc = jnp.transpose(vc_loc[0], (0, 1, 3, 4, 2)).reshape(layers, batch * slots * head_dim, t_len)
        steps = 8
        group_w = rep * head_dim

        (qkv,) = trunk(0, hidden, None, cos, sin, w_qkv, w_out, w_gate, w_up, w_down)
        caches = None
        kv_layers = []
        for layer in range(layers):
            kv_all = lax.all_gather(qkv[:p_rows, q_cols:], ('side', 'tp'), axis=0, tiled=True)
            kv_layers.append(kv_all)
            dec = qkv[p_rows:]
            dec_q = dec[:, :q_cols].reshape(d_rows, slots, tp, group_w)
            dec_k = dec[:, q_cols:q_cols + kv_cols].reshape(d_rows, slots, tp, head_dim)
            dec_v = dec[:, q_cols + kv_cols:].reshape(d_rows, slots, tp, head_dim)
            send = jnp.transpose(jnp.concatenate([dec_q, dec_k, dec_v], axis=3), (2, 0, 1, 3))
            got = lax.all_to_all(send, 'tp', 0, 0, tiled=True).reshape(batch, slots, group_w + 2 * head_dim)
            q_dec = got[:, :, :group_w].reshape(batch * slots * rep, head_dim)
            k_new = jnp.transpose(got[:, :, group_w:group_w + head_dim].reshape(steps, batch * slots // steps, head_dim), (0, 2, 1))
            v_new = jnp.transpose(got[:, :, group_w + head_dim:].reshape(steps, batch * slots // steps, head_dim), (0, 2, 1))
            ctx_p = prompt_attn(qkv[:p_rows, :q_cols], kv_all, key0, row0, seg_start[:, None].astype(jnp.int32), window, head_dim, rep)
            ctx_d, k_out, v_out = decode_attn(layer, q_dec, k_new, v_new, lengths, kc, vc, caches, head_dim, rep, slots, steps)
            caches = (k_out, v_out)
            back = lax.all_to_all(ctx_d.reshape(tp, d_rows, slots, group_w), 'tp', 0, 0, tiled=True)
            ctx = jnp.concatenate([ctx_p, jnp.transpose(back, (1, 2, 0, 3)).reshape(d_rows, q_cols)], axis=0)
            if layer + 1 < layers:
                hidden, qkv = trunk(layer, hidden, ctx, cos, sin, w_qkv, w_out, w_gate, w_up, w_down)
            else:
                (hidden,) = trunk(layer, hidden, ctx, None, None, w_qkv, w_out, w_gate, w_up, w_down)
        all_hidden = lax.all_gather(hidden, 'tp', axis=0)
        hidden_rows = all_hidden[:, :p_rows].reshape(prompt_rows, -1)
        dec_out = all_hidden[:, p_rows:].reshape(batch, -1)

        mine = dest == s_idx
        starts = ends - req_len
        start = jnp.sum(jnp.where(mine, starts, 0))
        length = jnp.sum(jnp.where(mine, req_len, 0))
        keep = (jnp.arange(max_req) < length)[None, :, None, None, None]
        full = jnp.stack(kv_layers).reshape(layers, seq_len, 2, slots, tp, head_dim)
        full = lax.dynamic_index_in_dim(full, t_idx, axis=4, keepdims=False)
        full = jnp.concatenate([full, jnp.zeros((layers, max_req) + full.shape[2:], BF16)], axis=1)
        piece = lax.dynamic_slice_in_dim(full, start, max_req, axis=1)
        piece = jnp.where(keep, piece, jnp.zeros_like(piece))

        def cache_back(arr):
            return jnp.transpose(arr.reshape(layers, batch, slots, head_dim, t_len), (0, 1, 4, 2, 3))[None]

        return hidden_rows, dec_out[None], piece[:, :, 0][None], piece[:, :, 1][None], cache_back(caches[0]), cache_back(caches[1])

    return jax.shard_map(local_step, mesh=mesh,
                         in_specs=(rows_spec, P('pair'), P('pair'), P(), P(), P(), P(), P(), batch_spec, cache_spec, cache_spec, rows_spec),
                         out_specs=(rows_spec, batch_spec, prompt_spec, prompt_spec, cache_spec, cache_spec),
                         check_vma=False)
```

```python
import functools

import jax
import jax.numpy as jnp
from jax import lax
from jax.experimental import pallas as pl
from jax.experimental.pallas import tpu as pltpu
from jax.sharding import PartitionSpec as P

ROPE_BASE = 10000.0
NORM_EPS = 1e-5
BF16 = jnp.bfloat16
F32 = jnp.float32
TILE = 512
W_SLOTS = 10
D_SLOTS = 6
CORES = 2
ANY = pl.BlockSpec(memory_space=pl.ANY)
VMEM = pl.BlockSpec(memory_space=pltpu.VMEM)
SMEM = pl.BlockSpec(memory_space=pltpu.SMEM)
MESH = pl.DeviceIdType.MESH
NT = (((1,), (1,)), ((), ()))


def rms(wide):
    return (wide * lax.rsqrt(jnp.mean(wide * wide, axis=-1, keepdims=True) + NORM_EPS)).astype(BF16)


def rope_tile(vals, cos, sin, head_dim):
    wide = vals.astype(F32)
    width = wide.shape[1]
    half = head_dim // 2
    lane = lax.broadcasted_iota(jnp.int32, wide.shape, 1)
    other = jnp.where(lax.rem(lane, head_dim) < half, pltpu.roll(wide, width - half, 1), pltpu.roll(wide, half, 1))
    reps = width // cos.shape[1]
    return (wide * jnp.concatenate([cos] * reps, axis=1) + other * jnp.concatenate([sin] * reps, axis=1)).astype(BF16)


def mega_kernel(cfg, x_ref, y_ref, cos_ref, sin_ref, seg_ref, cosd_ref, sind_ref, len_ref, kc_ref, vc_ref,
                wq_ref, wo_ref, wg_ref, wu_ref, wd_ref,
                hid_ref, dec_ref, inst_ref, knv_ref,
                wbuf, dbuf, hin, h_ref, norm_ref, acc, xch, qkv, kvwin, dsend, rdec, cback, ctx, isend, kbuf, vbuf, hfin, mask_ref,
                wsem, dsem, insem, csem, xsend, xrecv, kvs, kvr, dss, dsr, cbs, cbr, iss, isr, ilo, fhs, fhr, fds, fdr, flo):
    side, tp, layers, head_dim, rep, slots = cfg
    s_me = lax.axis_index('side')
    t_me = lax.axis_index('tp')
    core = lax.rem(s_me, CORES)
    col = s_me // CORES
    chip = col * tp + t_me
    chips = side // CORES * tp
    partner = s_me + 1 - 2 * core
    model = h_ref.shape[1]
    rows = h_ref.shape[0]
    p_rows = mask_ref.shape[0]
    d_rows = (rows - p_rows) // CORES
    half_p = p_rows // 2
    window = kvwin.shape[1]
    q_loc = ctx.shape[2]
    group_w = rep * head_dim
    heads = q_loc // group_w
    kv_loc = heads * head_dim
    q_all = wo_ref.shape[1]
    kv_all = (wq_ref.shape[2] - q_all) // 2
    ff_loc = wg_ref.shape[2] // CORES
    n_ff = ff_loc // TILE
    n_q = q_loc // TILE
    n_o = q_loc // TILE
    n_w = 1 + n_q + 2 * n_ff
    n_d = n_o + n_ff

    def rc(src, dst, ssem, rsem, s_dev, t_dev):
        return pltpu.make_async_remote_copy(src_ref=src, dst_ref=dst, send_sem=ssem, recv_sem=rsem,
                                            device_id={'side': s_dev, 'tp': t_dev}, device_id_type=MESH)

    def at(base, size, unit):
        return pl.ds(pl.multiple_of(base, unit), size)

    def w_copies(idx):
        layer, pos = divmod(idx, n_w)
        slot = idx % W_SLOTS
        dst = wbuf.at[slot]
        if pos == 0:
            return [pltpu.make_async_copy(wq_ref.at[layer, :, at(q_all + core * kv_loc, kv_loc, 128)], dst.at[:, pl.ds(0, kv_loc)], wsem.at[slot, 0]),
                    pltpu.make_async_copy(wq_ref.at[layer, :, at(q_all + kv_all + core * kv_loc, kv_loc, 128)], dst.at[:, pl.ds(kv_loc, kv_loc)], wsem.at[slot, 1])]
        if pos <= n_q:
            return [pltpu.make_async_copy(wq_ref.at[layer, :, at(core * q_loc + (pos - 1) * TILE, TILE, TILE)], dst, wsem.at[slot, 0])]
        pos -= 1 + n_q
        src = (wg_ref, wu_ref)[pos % 2]
        return [pltpu.make_async_copy(src.at[layer, :, at(core * ff_loc + (pos // 2) * TILE, TILE, TILE)], dst, wsem.at[slot, 0])]

    def d_copies(idx):
        layer, pos = divmod(idx, n_d)
        slot = idx % D_SLOTS
        if pos < n_o:
            src = wo_ref.at[layer, at(core * q_loc + pos * TILE, TILE, TILE), :]
        else:
            src = wd_ref.at[layer, at(core * ff_loc + (pos - n_o) * TILE, TILE, TILE), :]
        return [pltpu.make_async_copy(src, dbuf.at[slot], dsem.at[slot])]

    def start_all(copies):
        for one in copies:
            one.start()

    def wait_all(copies):
        for one in copies:
            one.wait()

    def w_next(idx):
        if idx + W_SLOTS < layers * n_w:
            start_all(w_copies(idx + W_SLOTS))

    def d_next(idx):
        if idx + D_SLOTS < layers * n_d:
            start_all(d_copies(idx + D_SLOTS))

    def cache_copies(layer):
        return [pltpu.make_async_copy(kc_ref.at[layer], kbuf, csem.at[0]), pltpu.make_async_copy(vc_ref.at[layer], vbuf, csem.at[1])]

    x_mine = core == t_me // (tp // CORES)
    x_src = x_ref.at[at(lax.rem(t_me, tp // CORES) * p_rows, p_rows, p_rows), :]
    x_dst = hin.at[pl.ds(0, p_rows), :]
    y_src = y_ref.at[at(t_me * d_rows, d_rows, d_rows), :]
    y_dst = hin.at[at(p_rows + core * d_rows, d_rows, d_rows), :]
    x_local = pltpu.make_async_copy(x_src, x_dst, insem.at[0])
    y_local = pltpu.make_async_copy(y_src, y_dst, insem.at[1])
    x_far = rc(x_src, x_dst, insem.at[2], insem.at[3], partner, t_me)
    y_far = rc(y_src, y_dst, insem.at[4], insem.at[5], partner, t_me)

    start_all(w_copies(0))

    @pl.when(x_mine)
    def _():
        x_local.start()

    y_local.start()
    for idx in range(1, W_SLOTS):
        start_all(w_copies(idx))
        if idx == 2:
            start_all(cache_copies(0))
            start_all(d_copies(0))
            start_all(d_copies(1))
    for idx in range(2, D_SLOTS):
        start_all(d_copies(idx))

    barrier = pltpu.get_barrier_semaphore()
    for ds in range(side):
        for dt in range(tp):
            if ds or dt:
                pl.semaphore_signal(barrier, inc=1, device_id={'side': lax.rem(s_me + ds, side), 'tp': lax.rem(t_me + dt, tp)}, device_id_type=MESH)

    for layer in range(layers):
        kvwin[layer, 0:half_p, :] = jnp.zeros((half_p, kvwin.shape[2]), BF16)
        for dist in range(1, window // p_rows):
            lo = window - p_rows * (dist + 1)
            lo = max(lo, half_p)

            @pl.when(chip < dist)
            def _():
                hi = window - p_rows * dist
                kvwin[layer, lo:hi, :] = jnp.zeros((hi - lo, kvwin.shape[2]), BF16)

    key_row = (chip + 1) * p_rows - window + lax.broadcasted_iota(jnp.int32, mask_ref.shape, 1)
    q_row = chip * p_rows + lax.broadcasted_iota(jnp.int32, mask_ref.shape, 0)
    mask_ref[...] = jnp.where((key_row <= q_row) & (key_row >= seg_ref[...]), 1.0, 0.0)

    pl.semaphore_wait(barrier, side * tp - 1)

    @pl.when(x_mine)
    def _():
        x_far.start()

    y_far.start()

    @pl.when(x_mine)
    def _():
        x_local.wait()

    @pl.when(jnp.logical_not(x_mine))
    def _():
        x_far.wait_recv()

    y_local.wait()
    y_far.wait_recv()
    h_ref[...] = hin[...].astype(F32)

    diag = (lax.broadcasted_iota(jnp.int32, (d_rows, d_rows * head_dim), 1) // head_dim) == lax.broadcasted_iota(jnp.int32, (d_rows, d_rows * head_dim), 0)
    scale = head_dim ** -0.5

    def exchange(idx):
        return rc(acc, xch.at[idx], xsend.at[idx], xrecv.at[idx], partner, t_me)

    for layer in range(layers):
        w_base = layer * n_w
        d_base = layer * n_d
        norm_ref[...] = rms(h_ref[...])
        cos = cos_ref[...]
        sin = sin_ref[...]

        wait_all(w_copies(w_base))
        out = jnp.dot(norm_ref[...], wbuf[w_base % W_SLOTS], preferred_element_type=F32).astype(BF16)
        w_next(w_base)
        qkv[:, q_loc:] = out
        kvwin[layer, window - p_rows:, 0:kv_loc] = rope_tile(out[:p_rows, :kv_loc], cos, sin, head_dim)
        kvwin[layer, window - p_rows:, kv_loc:] = out[:p_rows, kv_loc:]

        def halo(dist):
            target = chip + dist
            last = window - p_rows * dist
            size = p_rows if last - p_rows >= half_p else half_p
            src = kvwin.at[layer, pl.ds(window - size, size), :]
            dst = kvwin.at[layer, pl.ds(last - size, size), :]
            return rc(src, dst, kvs.at[layer, dist - 1], kvr.at[layer, dist - 1], CORES * (target // tp) + core, lax.rem(target, tp))

        for dist in range(1, window // p_rows):
            @pl.when(chip + dist < chips)
            def _():
                halo(dist).start()

        for tile in range(n_q):
            idx = w_base + 1 + tile
            wait_all(w_copies(idx))
            out = jnp.dot(norm_ref[...], wbuf[idx % W_SLOTS], preferred_element_type=F32).astype(BF16)
            w_next(idx)
            sl = slice(tile * TILE, (tile + 1) * TILE)
            qkv[:p_rows, sl] = rope_tile(out[:p_rows], cos, sin, head_dim)
            qkv[p_rows:, sl] = out[p_rows:]

        for sub in range(CORES):
            for head in range(heads):
                r0 = p_rows + sub * d_rows
                kk = qkv[r0:r0 + d_rows, q_loc + head * head_dim:q_loc + (head + 1) * head_dim]
                vv = qkv[r0:r0 + d_rows, q_loc + kv_loc + head * head_dim:q_loc + kv_loc + (head + 1) * head_dim]
                dsend[layer, sub, head, :, 0:group_w] = qkv[r0:r0 + d_rows, head * group_w:(head + 1) * group_w]
                dsend[layer, sub, head, :, group_w:] = jnp.concatenate([kk, vv], axis=1)

        def forward(dt, dc):
            s2 = lax.rem(core + dc, CORES)
            t2 = lax.rem(t_me + dt, tp)
            return rc(dsend.at[layer, s2, t2], rdec.at[layer, t_me, core], dss.at[layer, dt * CORES + dc], dsr.at[layer, dt * CORES + dc], col * CORES + s2, t2)

        for dt in range(tp):
            for dc in range(CORES):
                if dt or dc:
                    forward(dt, dc).start()
        rdec[layer, t_me, core] = dsend[layer, core, t_me]

        def backward(dt, dc):
            t2 = lax.rem(t_me + tp - dt, tp)
            c2 = lax.rem(core + dc, CORES)
            dst = ctx.at[layer, at(p_rows + core * d_rows, d_rows, d_rows), at(t_me * group_w, group_w, group_w)]
            return rc(cback.at[layer, dt * CORES + dc], dst, cbs.at[layer, dt * CORES + dc], cbr.at[layer, dt * CORES + dc], col * CORES + c2, t2)

        wait_all(cache_copies(layer))
        for dt in range(tp):
            for dc in range(CORES):
                t2 = lax.rem(t_me + tp - dt, tp)
                c2 = lax.rem(core + dc, CORES)
                if dt or dc:
                    forward(dt, dc).wait_recv()
                raw = rdec[layer, t2, c2]
                roped = rope_tile(raw, cosd_ref[t2], sind_ref[t2], head_dim)
                k_new = roped[:, group_w:group_w + head_dim]
                v_new = raw[:, group_w + head_dim:]
                knv_ref[layer, t2, c2] = jnp.concatenate([k_new, v_new], axis=1)
                q_wide = roped[:, :group_w].astype(F32) * scale
                q_parts = [q_wide[:, r * head_dim:(r + 1) * head_dim] for r in range(rep)]
                lhs = jnp.concatenate([jnp.where(diag, jnp.concatenate([jnp.concatenate([part, part], axis=1)] * (d_rows // 2), axis=1), 0.0) for part in q_parts], axis=0).astype(BF16)
                k_part = kbuf[at(t2 * d_rows, d_rows, d_rows), c2].reshape(d_rows * head_dim, kbuf.shape[3])
                v_part = vbuf[at(t2 * d_rows, d_rows, d_rows), c2].reshape(d_rows * head_dim, vbuf.shape[3])
                scores = jnp.dot(lhs, k_part, preferred_element_type=F32)
                s_new = jnp.sum(jnp.concatenate(q_parts, axis=0) * jnp.concatenate([k_new.astype(F32)] * rep, axis=0), axis=-1, keepdims=True)
                where_new = len_ref[t2]
                pos = lax.broadcasted_iota(jnp.int32, scores.shape, 1)
                scores = jnp.where(pos < where_new, scores, -1e30)
                scores = jnp.where(pos == where_new, s_new, scores)
                scores = jnp.exp(scores - jnp.max(scores, axis=-1, keepdims=True))
                prob = (scores * (1.0 / jnp.sum(scores, axis=-1, keepdims=True))).astype(BF16).astype(F32)
                p_new = jnp.sum(jnp.where(pos == where_new, prob, 0.0), axis=-1, keepdims=True)
                p_old = jnp.where(pos == where_new, 0.0, prob).astype(BF16)
                full = lax.dot_general(p_old, v_part, NT, preferred_element_type=F32)
                full = jnp.where(jnp.concatenate([diag] * rep, axis=0), full, 0.0)
                fold = full[:, 0:128]
                for piece in range(1, full.shape[1] // 128):
                    fold = fold + full[:, piece * 128:(piece + 1) * 128]
                got = fold[:, :head_dim] + fold[:, head_dim:] + p_new * jnp.concatenate([v_new.astype(F32)] * rep, axis=0)
                got = jnp.concatenate([got[r * d_rows:(r + 1) * d_rows] for r in range(rep)], axis=1).astype(BF16)
                if dt or dc:
                    cback[layer, dt * CORES + dc] = got
                    backward(dt, dc).start()
                else:
                    ctx[layer, at(p_rows + core * d_rows, d_rows, d_rows), at(t_me * group_w, group_w, group_w)] = got
        if layer + 1 < layers:
            start_all(cache_copies(layer + 1))

        for dist in range(1, window // p_rows):
            @pl.when(chip >= dist)
            def _():
                halo(dist).wait_recv()

        allowed = mask_ref[...] > 0.5
        for head in range(heads):
            k_head = kvwin[layer, :, head * head_dim:(head + 1) * head_dim]
            v_head = kvwin[layer, :, kv_loc + head * head_dim:kv_loc + (head + 1) * head_dim]
            outs = []
            for sub in range(rep):
                q0 = head * group_w + sub * head_dim
                q_part = (qkv[:p_rows, q0:q0 + head_dim].astype(F32) * scale).astype(BF16)
                scores = lax.dot_general(q_part, k_head, NT, preferred_element_type=F32)
                scores = jnp.where(allowed, scores, -1e30)
                scores = jnp.exp(scores - jnp.max(scores, axis=-1, keepdims=True))
                prob = (scores * (1.0 / jnp.sum(scores, axis=-1, keepdims=True))).astype(BF16)
                outs.append(jnp.dot(prob, v_head, preferred_element_type=F32).astype(BF16))
            ctx[layer, 0:p_rows, head * group_w:(head + 1) * group_w] = jnp.concatenate(outs, axis=1)
            isend[layer, head] = jnp.concatenate([k_head[window - p_rows:], v_head[window - p_rows:]], axis=1)

        def install(ds, dt):
            s2 = lax.rem(s_me + ds, side)
            t2 = lax.rem(t_me + dt, tp)
            return rc(isend.at[layer, t2], inst_ref.at[layer, core, at(chip * p_rows, p_rows, p_rows), :], iss.at[layer, ds * tp + dt], isr.at[layer, ds * tp + dt], s2, t2)

        def install_own():
            return pltpu.make_async_copy(isend.at[layer, t_me], inst_ref.at[layer, core, at(chip * p_rows, p_rows, p_rows), :], ilo.at[layer])

        for ds in range(side):
            for dt in range(tp):
                if ds or dt:
                    install(ds, dt).start()
        install_own().start()

        for dt in range(tp):
            for dc in range(CORES):
                if dt or dc:
                    backward(dt, dc).wait_recv()

        if layer:
            exchange(2 * layer - 1).wait_send()
        for tile in range(n_o):
            idx = d_base + tile
            wait_all(d_copies(idx))
            part = jnp.dot(ctx[layer, :, tile * TILE:(tile + 1) * TILE], dbuf[idx % D_SLOTS], preferred_element_type=F32)
            if tile == 0:
                acc[...] = part
            else:
                acc[...] += part
            d_next(idx)
        exchange(2 * layer).start()
        exchange(2 * layer).wait()
        h_ref[...] = (h_ref[...] + (acc[...] + xch[2 * layer]).astype(BF16).astype(F32)).astype(BF16).astype(F32)
        norm_ref[...] = rms(h_ref[...])

        for chunk in range(n_ff):
            idx = w_base + 1 + n_q + 2 * chunk
            wait_all(w_copies(idx))
            gate = jnp.dot(norm_ref[...], wbuf[idx % W_SLOTS], preferred_element_type=F32).astype(BF16).astype(F32)
            w_next(idx)
            wait_all(w_copies(idx + 1))
            upper = jnp.dot(norm_ref[...], wbuf[(idx + 1) % W_SLOTS], preferred_element_type=F32).astype(BF16).astype(F32)
            w_next(idx + 1)
            act = (jax.nn.silu(gate) * upper).astype(BF16)
            d_idx = d_base + n_o + chunk
            wait_all(d_copies(d_idx))
            part = jnp.dot(act, dbuf[d_idx % D_SLOTS], preferred_element_type=F32)
            if chunk == 0:
                acc[...] = part
            else:
                acc[...] += part
            d_next(d_idx)
        exchange(2 * layer + 1).start()
        exchange(2 * layer + 1).wait_recv()
        h_ref[...] = (h_ref[...] + (acc[...] + xch[2 * layer + 1]).astype(BF16).astype(F32)).astype(BF16).astype(F32)

        for dist in range(1, window // p_rows):
            @pl.when(chip + dist < chips)
            def _():
                halo(dist).wait_send()
        for dt in range(tp):
            for dc in range(CORES):
                if dt or dc:
                    forward(dt, dc).wait_send()
                    backward(dt, dc).wait_send()
        for ds in range(side):
            for dt in range(tp):
                if ds or dt:
                    install(ds, dt).wait()
        install_own().wait()

    exchange(2 * layers - 1).wait_send()

    @pl.when(x_mine)
    def _():
        x_far.wait_send()

    y_far.wait_send()

    hfin[...] = h_ref[...].astype(BF16)
    half_t = tp // CORES
    own_hid = core == t_me // half_t
    hid_src = hfin.at[at(core * half_p, half_p, half_p), :]
    hid_dst = hid_ref.at[at(lax.rem(t_me, half_t) * p_rows + core * half_p, half_p, half_p), :]
    dec_src = hfin.at[at(p_rows + core * d_rows, d_rows, d_rows), :]
    dec_dst = dec_ref.at[at(t_me * d_rows, d_rows, d_rows), :]
    hid_local = pltpu.make_async_copy(hid_src, hid_dst, flo.at[0])
    dec_local = pltpu.make_async_copy(dec_src, dec_dst, flo.at[1])
    piece_me = lax.rem(t_me, half_t) * CORES + core

    def hid_far(dt):
        return rc(hid_src, hid_dst, fhs.at[dt], fhr.at[piece_me], col * CORES + t_me // half_t, lax.rem(t_me + dt, tp))

    def dec_far(dt):
        return rc(dec_src, dec_dst, fds.at[dt], fdr.at[dt], s_me, lax.rem(t_me + dt, tp))

    for dt in range(1, tp):
        hid_far(dt).start()
        dec_far(dt).start()

    @pl.when(own_hid)
    def _():
        hid_local.start()

    @pl.when(jnp.logical_not(own_hid))
    def _():
        hid_far(0).start()

    dec_local.start()
    for dt in range(1, tp):
        hid_far(dt).wait_send()
        dec_far(dt).wait()

    @pl.when(own_hid)
    def _():
        hid_local.wait()

    @pl.when(jnp.logical_not(own_hid))
    def _():
        hid_far(0).wait_send()

    dec_local.wait()
    for sub in range(half_t):
        for c2 in range(CORES):
            mine = (core * half_t + sub == t_me) & (core == c2)

            @pl.when(jnp.logical_not(mine))
            def _():
                rc(hid_src, hid_ref.at[pl.ds(sub * p_rows + c2 * half_p, half_p), :], fhs.at[0], fhr.at[sub * CORES + c2], s_me, t_me).wait_recv()


def finish_kernel(head_dim, slots, blk_ref, len_ref, inst_ref, kn_ref, vn_ref, k_ref, v_ref, kp_ref, vp_ref, kout_ref, vout_ref, ibuf, isem):
    layer = pl.program_id(0)
    step = pl.program_id(1)
    t_len = k_ref.shape[1]
    pairs = k_ref.shape[0] // head_dim
    batch = pairs // slots
    win = ibuf.shape[1]
    max_req = kp_ref.shape[1]

    def grab(lay):
        return pltpu.make_async_copy(inst_ref.at[lay, :, pl.ds(pl.multiple_of(blk_ref[0], 16), win), :], ibuf, isem)

    @pl.when(step == 0)
    def _():
        grab(layer).start()

    t_iota = lax.broadcasted_iota(jnp.int32, (head_dim, t_len), 1)
    for pair in range(pairs):
        here = t_iota == len_ref[step * batch + pair // slots]
        sl = slice(pair * head_dim, (pair + 1) * head_dim)
        kout_ref[sl, :] = jnp.where(here, kn_ref[:, pair:pair + 1].astype(F32), k_ref[sl, :].astype(F32)).astype(BF16)
        vout_ref[sl, :] = jnp.where(here, vn_ref[:, pair:pair + 1].astype(F32), v_ref[sl, :].astype(F32)).astype(BF16)

    @pl.when(step == 0)
    def _():
        grab(layer).wait()
        row = blk_ref[0] + lax.broadcasted_iota(jnp.int32, (win, max_req), 0)
        want = lax.broadcasted_iota(jnp.int32, (win, max_req), 1)
        pick = jnp.where((row - blk_ref[1] == want) & (want < blk_ref[2]), 1.0, 0.0).astype(BF16)
        for slot in range(slots):
            both = lax.dot_general(ibuf[slot], pick, (((0,), (0,)), ((), ())), preferred_element_type=F32).astype(BF16)
            kp_ref[slot * head_dim:(slot + 1) * head_dim, :] = both[:head_dim]
            vp_ref[slot * head_dim:(slot + 1) * head_dim, :] = both[head_dim:]


def solution(mesh):
    tp = mesh.shape['tp']
    side = mesh.shape['side']
    rows_spec = P(('pair', 'side'), None)
    batch_spec = P(('pair', 'side'), None, None)
    cache_spec = P(('pair', 'side'), None, None, None, 'tp', None)
    prompt_spec = P(('pair', 'side'), None, None, 'tp', None)

    def local_step(x_loc, req_len, dest, w_qkv, w_out, w_gate, w_up, w_down, y_loc, kc_loc, vc_loc, clen_loc):
        s_idx = lax.axis_index('side')
        t_idx = lax.axis_index('tp')
        layers = w_qkv.shape[0]
        head_dim = kc_loc.shape[-1]
        slots = kc_loc.shape[-2]
        t_len = kc_loc.shape[3]
        batch = y_loc.shape[1]
        kv_heads = slots * tp
        rep = w_out.shape[1] // head_dim // kv_heads
        model = x_loc.shape[1]
        prompt_rows = x_loc.shape[0]
        seq_len = prompt_rows * side
        max_req = 2 * prompt_rows - prompt_rows // 4
        p_rows = prompt_rows * CORES // tp
        d_rows = batch // tp
        rows = p_rows + CORES * d_rows
        q_loc = w_out.shape[1] // CORES
        kv_loc = kv_heads // CORES * head_dim
        heads = kv_heads // CORES
        window = -(-(max_req - 1) // p_rows) * p_rows + p_rows
        group_w = rep * head_dim

        chip = s_idx // CORES * tp + t_idx
        ids = jnp.arange(side)
        ends = jnp.sum(jnp.where(ids[None, :] <= ids[:, None], req_len[None, :], 0), axis=1)
        row_ids = chip * p_rows + jnp.arange(p_rows)
        seg_start = jnp.sum(jnp.where(row_ids[:, None] >= ends[None, :], req_len[None, :], 0), axis=1)
        lengths = clen_loc[0]
        half = head_dim // 2
        inv_freq = ROPE_BASE ** (-jnp.arange(half, dtype=F32) / half)
        positions = jnp.concatenate([row_ids - seg_start, lengths])
        angles = positions.astype(F32)[:, None] * inv_freq
        cos = jnp.cos(angles)
        sin = jnp.sin(angles)
        cos = jnp.concatenate([cos] * 4, axis=1)
        sin = jnp.concatenate([-sin, sin] * 2, axis=1)
        cos_d = cos[p_rows:].reshape(tp, d_rows, 2 * head_dim)
        sin_d = sin[p_rows:].reshape(tp, d_rows, 2 * head_dim)
        len_rows = jnp.broadcast_to(lengths.reshape(tp, 1, d_rows), (tp, rep, d_rows)).reshape(tp, rep * d_rows, 1)
        kc = jnp.transpose(kc_loc[0], (0, 1, 3, 4, 2))
        vc = jnp.transpose(vc_loc[0], (0, 1, 3, 4, 2))

        dma = pltpu.SemaphoreType.DMA
        n_peer = tp * CORES
        hid, dec, inst, knv = pl.pallas_call(
            functools.partial(mega_kernel, (side, tp, layers, head_dim, rep, slots)),
            out_shape=[jax.ShapeDtypeStruct((prompt_rows, model), BF16), jax.ShapeDtypeStruct((batch, model), BF16),
                       jax.ShapeDtypeStruct((layers, CORES, seq_len, 2 * head_dim), BF16),
                       jax.ShapeDtypeStruct((layers, tp, CORES, d_rows, 2 * head_dim), BF16)],
            in_specs=[ANY, ANY, VMEM, VMEM, VMEM, VMEM, VMEM, VMEM, ANY, ANY, ANY, ANY, ANY, ANY, ANY],
            out_specs=[ANY, ANY, ANY, VMEM],
            scratch_shapes=[
                pltpu.VMEM((W_SLOTS, model, TILE), BF16),
                pltpu.VMEM((D_SLOTS, TILE, model), BF16),
                pltpu.VMEM((rows, model), BF16),
                pltpu.VMEM((rows, model), F32),
                pltpu.VMEM((rows, model), BF16),
                pltpu.VMEM((rows, model), F32),
                pltpu.VMEM((2 * layers, rows, model), F32),
                pltpu.VMEM((rows, q_loc + 2 * kv_loc), BF16),
                pltpu.VMEM((layers, window, 2 * kv_loc), BF16),
                pltpu.VMEM((layers, CORES, heads, d_rows, group_w + 2 * head_dim), BF16),
                pltpu.VMEM((layers, tp, CORES, d_rows, group_w + 2 * head_dim), BF16),
                pltpu.VMEM((layers, n_peer, d_rows, group_w), BF16),
                pltpu.VMEM((layers, rows, q_loc), BF16),
                pltpu.VMEM((layers, heads, p_rows, 2 * head_dim), BF16),
                pltpu.VMEM((batch, slots, head_dim, t_len), BF16),
                pltpu.VMEM((batch, slots, head_dim, t_len), BF16),
                pltpu.VMEM((rows, model), BF16),
                pltpu.VMEM((p_rows, window), F32),
                dma((W_SLOTS, 2)), dma((D_SLOTS,)), dma((6,)), dma((2,)),
                dma((2 * layers,)), dma((2 * layers,)),
                dma((layers, 4)), dma((layers, 4)),
                dma((layers, n_peer)), dma((layers, n_peer)),
                dma((layers, n_peer)), dma((layers, n_peer)),
                dma((layers, side * tp)), dma((layers, side * tp)), dma((layers,)),
                dma((tp,)), dma((tp,)), dma((tp,)), dma((tp,)), dma((2,)),
            ],
            compiler_params=pltpu.CompilerParams(collective_id=0, has_side_effects=True, vmem_limit_bytes=67043328),
            name="mega",
        )(x_loc, y_loc[0], cos[:p_rows], sin[:p_rows], seg_start[:, None].astype(jnp.int32), cos_d, sin_d, len_rows, kc, vc,
          w_qkv, w_out, w_gate, w_up, w_down)

        mine = dest == s_idx
        start = jnp.sum(jnp.where(mine, ends - req_len, 0))
        length = jnp.sum(jnp.where(mine, req_len, 0))
        win = 512
        blk = jnp.minimum(start // 64 * 64, seq_len - win)
        steps = 8
        depth = batch * slots * head_dim
        per = batch * slots // steps
        new = jnp.transpose(knv, (0, 1, 3, 2, 4)).reshape(layers, steps, per, 2 * head_dim)
        new = jnp.transpose(new, (0, 1, 3, 2))
        kc2 = kc.reshape(layers, depth, t_len)
        vc2 = vc.reshape(layers, depth, t_len)
        cache_b = pl.BlockSpec((None, depth // steps, t_len), lambda l, i: (l, i, 0))
        prompt_b = pl.BlockSpec((None, slots * head_dim, max_req), lambda l, i: (l, 0, 0))

        def col_b(which):
            return pl.BlockSpec((None, None, head_dim, per), lambda l, i: (l, i, which, 0))

        kp, vp, k_out, v_out = pl.pallas_call(
            functools.partial(finish_kernel, head_dim, slots),
            out_shape=[jax.ShapeDtypeStruct((layers, slots * head_dim, max_req), BF16)] * 2 + [jax.ShapeDtypeStruct(kc2.shape, BF16)] * 2,
            grid=(layers, steps),
            in_specs=[SMEM, SMEM, ANY, col_b(0), col_b(1), cache_b, cache_b],
            out_specs=[prompt_b, prompt_b, cache_b, cache_b],
            scratch_shapes=[pltpu.VMEM((slots, win, 2 * head_dim), BF16), dma],
            compiler_params=pltpu.CompilerParams(vmem_limit_bytes=40 * 2**20),
            name="finish",
        )(jnp.stack([blk, start, length]).astype(jnp.int32), lengths, inst, new, new, kc2, vc2)

        def cache_back(arr):
            return jnp.transpose(arr.reshape(layers, batch, slots, head_dim, t_len), (0, 1, 4, 2, 3))[None]

        def prompt_back(arr):
            return jnp.transpose(arr.reshape(layers, slots, head_dim, max_req), (0, 3, 1, 2))[None]

        return hid, dec[None], prompt_back(kp), prompt_back(vp), cache_back(k_out), cache_back(v_out)

    return jax.shard_map(local_step, mesh=mesh,
                         in_specs=(rows_spec, P('pair'), P('pair'), P(), P(), P(), P(), P(), batch_spec, cache_spec, cache_spec, rows_spec),
                         out_specs=(rows_spec, batch_spec, prompt_spec, prompt_spec, cache_spec, cache_spec),
                         check_vma=False)
```

```python
import functools
import math

import jax
import jax.numpy as jnp
from jax import lax
from jax.experimental import pallas as pl
from jax.experimental.pallas import tpu as pltpu
from jax.sharding import PartitionSpec as P

ROPE_BASE = 10000.0
NORM_EPS = 1e-5
BF16 = jnp.bfloat16
F32 = jnp.float32
TILE = 512
W_SLOTS = 18
CORES = 2
ANY = pl.BlockSpec(memory_space=pl.ANY)
VMEM = pl.BlockSpec(memory_space=pltpu.VMEM)
SMEM = pl.BlockSpec(memory_space=pltpu.SMEM)
MESH = pl.DeviceIdType.MESH
NT = (((1,), (1,)), ((), ()))


def rms(wide):
    return (wide * lax.rsqrt(jnp.mean(wide * wide, axis=-1, keepdims=True) + NORM_EPS)).astype(BF16)


def rope_tile(vals, cos, sin, head_dim):
    wide = vals.astype(F32)
    width = wide.shape[1]
    half = head_dim // 2
    lane = lax.broadcasted_iota(jnp.int32, wide.shape, 1)
    other = jnp.where(lax.rem(lane, head_dim) < half, pltpu.roll(wide, width - half, 1), pltpu.roll(wide, half, 1))
    reps = width // cos.shape[1]
    return (wide * jnp.concatenate([cos] * reps, axis=1) + other * jnp.concatenate([sin] * reps, axis=1)).astype(BF16)


def to_column(row, count, owner):
    n = row.shape[1]
    j = lax.broadcasted_iota(jnp.int32, (count, n), 0)
    return jnp.sum(jnp.where(lax.broadcasted_iota(jnp.int32, (count, n), 1) == owner(j), row.astype(F32), 0.0), axis=-1, keepdims=True)


def mega_kernel(cfg, req_ref, clen_ref, x_ref, y_ref, kc_ref, vc_ref, wq_ref, wo_ref, wg_ref, wu_ref, wd_ref,
                hid_ref, dec_ref, inst_ref, knv_ref,
                wbuf, hin, h_ref, norm_ref, acc, xch, qkv, kvwin, dsend, rdec, cback, ctx, isend, kbuf, vbuf, act_ref, gu, mask_ref, cos_ref, sin_ref, cosd_ref, sind_ref, len_ref,
                wsem, insem, csem, xsend, xrecv, kvs, kvr, dss, dsr, cbs, cbr, i1s, i1r, i2s, i2r, i3s, i3r, ilo, fhs, fhr, fds, fdr, hws, dws, flo):
    side, tp, layers, head_dim, rep, slots = cfg
    s_me = lax.axis_index('side')
    t_me = lax.axis_index('tp')
    core = lax.rem(s_me, CORES)
    col = s_me // CORES
    chip = col * tp + t_me
    chips = side // CORES * tp
    partner = s_me + 1 - 2 * core
    model = h_ref.shape[1]
    rows = h_ref.shape[0]
    p_rows = mask_ref.shape[0]
    d_rows = (rows - p_rows) // CORES
    half_p = p_rows // 2
    window = kvwin.shape[1]
    q_loc = ctx.shape[2]
    group_w = rep * head_dim
    heads = q_loc // group_w
    kv_loc = heads * head_dim
    q_all = wo_ref.shape[1]
    kv_all = (wq_ref.shape[2] - q_all) // 2
    ff_loc = wg_ref.shape[2] // CORES
    n_ff = ff_loc // TILE
    n_q = q_loc // TILE
    n_o = model * q_loc // (TILE * model)
    n_deep = ff_loc // model
    n_dn = model // TILE
    base_o = 1 + n_q
    base_g = base_o + n_o
    base_d = base_g + 2 * n_ff
    n_w = base_d + n_dn * n_deep

    def rc(src, dst, ssem, rsem, s_dev, t_dev):
        return pltpu.make_async_remote_copy(src_ref=src, dst_ref=dst, send_sem=ssem, recv_sem=rsem,
                                            device_id={'side': s_dev, 'tp': t_dev}, device_id_type=MESH)

    def at(base, size, unit):
        return pl.ds(pl.multiple_of(base, unit), size)

    def w_copies(idx):
        layer, pos = divmod(idx, n_w)
        slot = idx % W_SLOTS
        dst = wbuf.at[slot]
        if pos == 0:
            return [pltpu.make_async_copy(wq_ref.at[layer, :, at(q_all + core * kv_loc, kv_loc, 128)], dst.at[:, pl.ds(0, kv_loc)], wsem.at[slot, 0]),
                    pltpu.make_async_copy(wq_ref.at[layer, :, at(q_all + kv_all + core * kv_loc, kv_loc, 128)], dst.at[:, pl.ds(kv_loc, kv_loc)], wsem.at[slot, 1])]
        if pos < base_o:
            return [pltpu.make_async_copy(wq_ref.at[layer, :, at(core * q_loc + (pos - 1) * TILE, TILE, TILE)], dst, wsem.at[slot, 0])]
        if pos < base_g:
            pos -= base_o
            return [pltpu.make_async_copy(wo_ref.at[layer, at(core * q_loc, q_loc, q_loc), pl.ds((2 * pos + part) * TILE, TILE)], dst.at[pl.ds(part * q_loc, q_loc), :], wsem.at[slot, part]) for part in range(2)]
        if pos < base_d:
            pos -= base_g
            src = (wg_ref, wu_ref)[pos % 2]
            return [pltpu.make_async_copy(src.at[layer, :, at(core * ff_loc + (pos // 2) * TILE, TILE, TILE)], dst, wsem.at[slot, 0])]
        pos -= base_d
        return [pltpu.make_async_copy(wd_ref.at[layer, at(core * ff_loc + pos % n_deep * model, model, model), pl.ds(pos // n_deep * TILE, TILE)], dst, wsem.at[slot, 0])]

    def start_all(copies):
        for one in copies:
            one.start()

    def wait_all(copies):
        for one in copies:
            one.wait()

    def w_next(idx):
        if idx + W_SLOTS < layers * n_w:
            start_all(w_copies(idx + W_SLOTS))

    def cache_copies(layer):
        return [pltpu.make_async_copy(kc_ref.at[layer], kbuf, csem.at[0]), pltpu.make_async_copy(vc_ref.at[layer], vbuf, csem.at[1])]

    x_mine = core == t_me // (tp // CORES)
    x_src = x_ref.at[at(lax.rem(t_me, tp // CORES) * p_rows, p_rows, p_rows), :]
    x_dst = hin.at[pl.ds(0, p_rows), :]
    y_src = y_ref.at[at(t_me * d_rows, d_rows, d_rows), :]
    y_dst = hin.at[at(p_rows + core * d_rows, d_rows, d_rows), :]
    x_local = pltpu.make_async_copy(x_src, x_dst, insem.at[0])
    y_local = pltpu.make_async_copy(y_src, y_dst, insem.at[1])
    x_far = rc(x_dst, x_dst, insem.at[2], insem.at[3], partner, t_me)
    y_far = rc(y_dst, y_dst, insem.at[4], insem.at[5], partner, t_me)

    @pl.when(x_mine)
    def _():
        x_local.start()

    y_local.start()
    start_all(w_copies(0))

    barrier = pltpu.get_barrier_semaphore()
    for ds in range(side):
        for dt in range(tp):
            if ds or dt:
                pl.semaphore_signal(barrier, inc=1, device_id={'side': lax.rem(s_me + ds, side), 'tp': lax.rem(t_me + dt, tp)}, device_id_type=MESH)

    for idx in range(1, W_SLOTS):
        start_all(w_copies(idx))
        if idx == 2:
            start_all(cache_copies(0))

    for layer in range(layers):
        kvwin[layer, 0:half_p, :] = jnp.zeros((half_p, kvwin.shape[2]), BF16)
        for dist in range(1, window // p_rows):
            lo = max(window - p_rows * (dist + 1), half_p)

            @pl.when(chip < dist)
            def _():
                hi = window - p_rows * dist
                kvwin[layer, lo:hi, :] = jnp.zeros((hi - lo, kvwin.shape[2]), BF16)

    gu[...] = jnp.zeros_like(gu)

    lane = lax.broadcasted_iota(jnp.int32, (p_rows, 2 * head_dim), 1)
    freq = jnp.exp((lane & (head_dim // 2 - 1)).astype(F32) * (-math.log(ROPE_BASE) / (head_dim // 2)))
    sign = jnp.where((lane & (head_dim - 1)) < head_dim // 2, -1.0, 1.0)
    q_row = chip * p_rows + lax.broadcasted_iota(jnp.int32, (p_rows, 2 * head_dim), 0)
    seg = jnp.zeros_like(q_row)
    end = req_ref[0] * 0
    for req in range(side):
        end = end + req_ref[req]
        seg = seg + jnp.where(q_row >= end, req_ref[req], 0)
    angles = (q_row - seg).astype(F32) * freq
    cos_ref[...] = jnp.cos(angles)
    sin_ref[...] = jnp.sin(angles) * sign
    dec_pos = to_column(clen_ref[...], tp * CORES * d_rows, lambda j: (j // (CORES * d_rows)) * d_rows + (j & (d_rows - 1)))
    angles = dec_pos * freq
    cosd_ref[...] = jnp.cos(angles)
    sind_ref[...] = jnp.sin(angles) * sign
    len_ref[...] = to_column(clen_ref[...], tp * CORES * rep * d_rows, lambda j: (j // (CORES * rep * d_rows)) * d_rows + (j & (d_rows - 1))).astype(jnp.int32)
    for piece in range(window // (2 * head_dim)):
        key_row = (chip + 1) * p_rows - window + piece * 2 * head_dim + lane
        mask_ref[:, piece * 2 * head_dim:(piece + 1) * 2 * head_dim] = jnp.where((key_row <= q_row) & (key_row >= seg), 1.0, 0.0)

    pl.semaphore_wait(barrier, side * tp - 1)

    y_local.wait()
    y_far.start()

    @pl.when(x_mine)
    def _():
        x_local.wait()
        x_far.start()

    @pl.when(jnp.logical_not(x_mine))
    def _():
        x_far.wait_recv()

    y_far.wait_recv()
    h_ref[...] = hin[...].astype(F32)

    diag = (lax.broadcasted_iota(jnp.int32, (d_rows, d_rows * head_dim), 1) // head_dim) == lax.broadcasted_iota(jnp.int32, (d_rows, d_rows * head_dim), 0)
    scale = head_dim ** -0.5
    n_peer = tp * CORES

    def exchange(idx, grp):
        sl = at(grp * TILE, TILE, TILE)
        return rc(acc.at[:, sl], xch.at[idx, :, sl], xsend.at[idx, grp], xrecv.at[idx, grp], partner, t_me)

    def settle(idx, grp):
        exchange(idx, grp).wait()
        sl = at(grp * TILE, TILE, TILE)
        h_ref[:, sl] = (h_ref[:, sl] + (acc[:, sl] + xch[idx, :, sl]).astype(BF16).astype(F32)).astype(BF16).astype(F32)

    half_t = tp // CORES
    own_hid = core == t_me // half_t
    piece_me = lax.rem(t_me, half_t) * CORES + core
    n_groups = model // TILE

    def group(ref, base, size, unit, grp):
        return ref.at[at(base, size, unit), at(grp * TILE, TILE, TILE)]

    def hid_src(grp):
        return group(hin, core * half_p, half_p, half_p, grp)

    def hid_dst(grp):
        return group(hid_ref, lax.rem(t_me, half_t) * p_rows + core * half_p, half_p, half_p, grp)

    def hid_local(grp):
        return pltpu.make_async_copy(hid_src(grp), hid_dst(grp), flo.at[0, grp])

    def hid_far(grp, dt):
        return rc(hid_src(grp), hid_dst(grp), fhs.at[grp, dt], fhr.at[grp, piece_me], col * CORES + t_me // half_t, lax.rem(t_me + dt, tp))

    def dec_src(grp):
        return group(hin, p_rows + core * d_rows, d_rows, d_rows, grp)

    def dec_dst(grp):
        return group(dec_ref, t_me * d_rows, d_rows, d_rows, grp)

    def dec_local(grp):
        return pltpu.make_async_copy(dec_src(grp), dec_dst(grp), flo.at[1, grp])

    def dec_far(grp, dt):
        return rc(dec_src(grp), dec_dst(grp), fds.at[grp, dt], fdr.at[grp, dt], s_me, lax.rem(t_me + dt, tp))

    near = (1, tp - 1)

    def send_group(grp):
        sl = at(grp * TILE, TILE, TILE)
        hin[:, sl] = h_ref[:, sl].astype(BF16)
        for dt in near:
            hid_far(grp, dt).start()
            dec_far(grp, dt).start()

        @pl.when(own_hid)
        def _():
            hid_local(grp).start()

        @pl.when(jnp.logical_not(own_hid))
        def _():
            hid_far(grp, 0).start()

        dec_local(grp).start()

    partners = []
    for layer in range(layers):
        w_base = layer * n_w
        norm_ref[...] = rms(h_ref[...])
        cos = cos_ref[...]
        sin = sin_ref[...]

        wait_all(w_copies(w_base))
        out = jnp.dot(norm_ref[...], wbuf[(w_base) % W_SLOTS], preferred_element_type=F32).astype(BF16)
        w_next(w_base)
        qkv[:, q_loc:] = out
        kvwin[layer, window - p_rows:, 0:kv_loc] = rope_tile(out[:p_rows, :kv_loc], cos, sin, head_dim)
        kvwin[layer, window - p_rows:, kv_loc:] = out[:p_rows, kv_loc:]

        def halo(dist):
            target = chip + dist
            last = window - p_rows * dist
            size = p_rows if last - p_rows >= half_p else half_p
            src = kvwin.at[layer, pl.ds(window - size, size), :]
            dst = kvwin.at[layer, pl.ds(last - size, size), :]
            return rc(src, dst, kvs.at[layer, dist - 1], kvr.at[layer, dist - 1], CORES * (target // tp) + core, lax.rem(target, tp))

        for dist in range(1, window // p_rows):
            if dist <= 2:
                @pl.when(chip + dist < chips)
                def _():
                    halo(dist).start()

        for tile in range(n_q):
            idx = w_base + 1 + tile
            wait_all(w_copies(idx))
            out = jnp.dot(norm_ref[...], wbuf[idx % W_SLOTS], preferred_element_type=F32).astype(BF16)
            w_next(idx)
            sl = slice(tile * TILE, (tile + 1) * TILE)
            qkv[:p_rows, sl] = rope_tile(out[:p_rows], cos, sin, head_dim)
            qkv[p_rows:, sl] = out[p_rows:]

        for sub in range(CORES):
            for head in range(heads):
                r0 = p_rows + sub * d_rows
                kk = qkv[r0:r0 + d_rows, q_loc + head * head_dim:q_loc + (head + 1) * head_dim]
                vv = qkv[r0:r0 + d_rows, q_loc + kv_loc + head * head_dim:q_loc + kv_loc + (head + 1) * head_dim]
                dsend[layer, sub, head, :, 0:group_w] = qkv[r0:r0 + d_rows, head * group_w:(head + 1) * group_w]
                dsend[layer, sub, head, :, group_w:] = jnp.concatenate([kk, vv], axis=1)

        def forward(dt, dc):
            s2 = lax.rem(core + dc, CORES)
            t2 = lax.rem(t_me + dt, tp)
            return rc(dsend.at[layer, s2, t2], rdec.at[layer, t_me, core], dss.at[layer, dt * CORES + dc], dsr.at[layer, dt * CORES + dc], col * CORES + s2, t2)

        peers = [(dt, dc) for dt in range(tp) for dc in range(CORES) if dt or dc]
        for dt, dc in peers:
            forward(dt, dc).start()
        rdec[layer, t_me, core] = dsend[layer, core, t_me]
        for dist in range(1, window // p_rows):
            if dist > 2:
                @pl.when(chip + dist < chips)
                def _():
                    halo(dist).start()

        def backward(dt, dc):
            t2 = lax.rem(t_me + tp - dt, tp)
            c2 = lax.rem(core + dc, CORES)
            dst = ctx.at[layer, at(p_rows + core * d_rows, d_rows, d_rows), at(t_me * group_w, group_w, group_w)]
            return rc(cback.at[layer, t2 * CORES + c2], dst, cbs.at[layer, dt * CORES + dc], cbr.at[layer, dt * CORES + dc], col * CORES + c2, t2)

        wait_all(cache_copies(layer))
        for dt, dc in peers:
            forward(dt, dc).wait_recv()
        raw = jnp.concatenate([rdec[layer, p // CORES, p % CORES] for p in range(n_peer)], axis=0)
        roped = rope_tile(raw, cosd_ref[...], sind_ref[...], head_dim)
        q_wide = roped[:, :group_w].astype(F32) * scale
        k_new = roped[:, group_w:group_w + head_dim].astype(F32)
        v_new = raw[:, group_w + head_dim:].astype(F32)
        eye = jnp.where(lax.broadcasted_iota(jnp.int32, (d_rows, d_rows), 0) == lax.broadcasted_iota(jnp.int32, (d_rows, d_rows), 1), 1.0, 0.0).astype(BF16)
        both = jnp.concatenate([k_new, v_new], axis=1).astype(BF16)
        scores = []
        fresh = []
        for p in range(n_peer):
            rs = slice(p * d_rows, (p + 1) * d_rows)
            knv_ref[layer, p // CORES, p % CORES] = lax.dot_general(both[rs], eye, (((0,), (0,)), ((), ())), preferred_element_type=F32).astype(BF16)
            q_parts = [q_wide[rs, r * head_dim:(r + 1) * head_dim] for r in range(rep)]
            pairs = [jnp.concatenate([part, part], axis=1) for part in q_parts]
            lhs = jnp.concatenate([jnp.where(diag, jnp.concatenate([pair] * (d_rows // 2), axis=1), 0.0) for pair in pairs], axis=0).astype(BF16)
            y2 = p // CORES
            k_part = kbuf[y2 * d_rows:(y2 + 1) * d_rows, p % CORES].reshape(d_rows * head_dim, kbuf.shape[3])
            scores.append(jnp.dot(lhs, k_part, preferred_element_type=F32))
            fresh.append(jnp.concatenate(q_parts, axis=0) * jnp.concatenate([k_new[rs]] * rep, axis=0))
        scores = jnp.concatenate(scores, axis=0)
        s_new = jnp.sum(jnp.concatenate(fresh, axis=0), axis=-1, keepdims=True)
        where_new = len_ref[...]
        pos = lax.broadcasted_iota(jnp.int32, scores.shape, 1)
        scores = jnp.where(pos < where_new, scores, -1e30)
        scores = jnp.where(pos == where_new, s_new, scores)
        scores = jnp.exp(scores - jnp.max(scores, axis=-1, keepdims=True))
        prob = (scores * (1.0 / jnp.sum(scores, axis=-1, keepdims=True))).astype(BF16).astype(F32)
        p_new = jnp.sum(jnp.where(pos == where_new, prob, 0.0), axis=-1, keepdims=True)
        p_old = jnp.where(pos == where_new, 0.0, prob).astype(BF16)
        grp_rows = rep * d_rows
        for p in range(n_peer):
            y2 = p // CORES
            gs = slice(p * grp_rows, (p + 1) * grp_rows)
            v_part = vbuf[y2 * d_rows:(y2 + 1) * d_rows, p % CORES].reshape(d_rows * head_dim, vbuf.shape[3])
            full = lax.dot_general(p_old[gs], v_part, NT, preferred_element_type=F32)
            full = jnp.where(jnp.concatenate([diag] * rep, axis=0), full, 0.0)
            fold = full[:, 0:128]
            for piece in range(1, full.shape[1] // 128):
                fold = fold + full[:, piece * 128:(piece + 1) * 128]
            got = fold[:, :head_dim] + fold[:, head_dim:] + p_new[gs] * jnp.concatenate([v_new[p * d_rows:(p + 1) * d_rows]] * rep, axis=0)
            cback[layer, p] = jnp.concatenate([got[r * d_rows:(r + 1) * d_rows] for r in range(rep)], axis=1).astype(BF16)
        for dt, dc in peers:
            backward(dt, dc).start()
        ctx[layer, at(p_rows + core * d_rows, d_rows, d_rows), at(t_me * group_w, group_w, group_w)] = cback[layer, t_me * CORES + core]
        if layer + 1 < layers:
            start_all(cache_copies(layer + 1))

        for dist in range(1, window // p_rows):
            @pl.when(chip >= dist)
            def _():
                halo(dist).wait_recv()

        allowed = mask_ref[...] > 0.5
        for head in range(heads):
            k_head = kvwin[layer, :, head * head_dim:(head + 1) * head_dim]
            v_head = kvwin[layer, :, kv_loc + head * head_dim:kv_loc + (head + 1) * head_dim]
            q0 = head * group_w
            outs = []
            for pair in range(rep // 2):
                q_part = jnp.concatenate([qkv[:p_rows, q0 + sub * head_dim:q0 + (sub + 1) * head_dim] for sub in (2 * pair, 2 * pair + 1)], axis=0)
                q_part = (q_part.astype(F32) * scale).astype(BF16)
                scores = lax.dot_general(q_part, k_head, NT, preferred_element_type=F32).reshape(2, p_rows, window)
                scores = jnp.where(allowed[None], scores, -1e30)
                scores = jnp.exp(scores - jnp.max(scores, axis=-1, keepdims=True))
                prob = (scores * (1.0 / jnp.sum(scores, axis=-1, keepdims=True))).astype(BF16).reshape(2 * p_rows, window)
                got = jnp.dot(prob, v_head, preferred_element_type=F32).astype(BF16)
                outs += [got[:p_rows], got[p_rows:]]
            ctx[layer, 0:p_rows, q0:q0 + group_w] = jnp.concatenate(outs, axis=1)
            isend[layer, head] = jnp.concatenate([k_head[window - p_rows:], v_head[window - p_rows:]], axis=1)

        def spread(dt):
            t2 = lax.rem(t_me + dt, tp)
            return rc(isend.at[layer, t2], inst_ref.at[layer, core, at(chip * p_rows, p_rows, p_rows), :], i1s.at[layer, dt], i1r.at[layer, dt], s_me, t2)

        def keep_own():
            return pltpu.make_async_copy(isend.at[layer, t_me], inst_ref.at[layer, core, at(chip * p_rows, p_rows, p_rows), :], ilo.at[layer])

        def across(dx):
            part = inst_ref.at[layer, core, at(col * tp * p_rows, tp * p_rows, tp * p_rows), :]
            return rc(part, part, i2s.at[layer, dx], i2r.at[layer, dx], lax.rem(col + dx, side // CORES) * CORES + core, t_me)

        def to_partner(layer=layer):
            return rc(inst_ref.at[layer, core], inst_ref.at[layer, core], i3s.at[layer], i3r.at[layer], partner, t_me)

        partners.append(to_partner)
        for dt in range(1, tp):
            spread(dt).start()
        keep_own().start()
        for dt, dc in peers:
            backward(dt, dc).wait_recv()

        for tile in range(n_o):
            idx = w_base + base_o + tile
            wait_all(w_copies(idx))
            for part in range(2):
                lo = (2 * tile + part) * TILE
                acc[:, lo:lo + TILE] = jnp.dot(ctx[layer], wbuf[idx % W_SLOTS, part * q_loc:(part + 1) * q_loc, :], preferred_element_type=F32)
                exchange(2 * layer, 2 * tile + part).start()
            w_next(idx)
        for grp in range(n_groups):
            settle(2 * layer, grp)
        norm_ref[...] = rms(h_ref[...])

        for dt in range(1, tp):
            spread(dt).wait()
        keep_own().wait()
        for dx in range(1, side // CORES):
            across(dx).start()

        def wait_slot(slot):
            pltpu.make_async_copy(wg_ref.at[layer, :, pl.ds(0, TILE)], wbuf.at[slot], wsem.at[slot, 0]).wait()

        def silu_mul(chunk):
            act_ref[:, at(chunk * TILE, TILE, TILE)] = (jax.nn.silu(gu[0].astype(F32)) * gu[1].astype(F32)).astype(BF16)

        def gate_up(chunk, carry):
            slot_g = lax.rem(w_base + base_g + 2 * chunk, W_SLOTS)
            slot_u = lax.rem(w_base + base_g + 2 * chunk + 1, W_SLOTS)
            wait_slot(slot_g)
            wait_slot(slot_u)
            gate = jnp.dot(norm_ref[...], wbuf[slot_g], preferred_element_type=F32).astype(BF16)
            silu_mul(jnp.maximum(chunk - 1, 0))
            upper = jnp.dot(norm_ref[...], wbuf[slot_u], preferred_element_type=F32).astype(BF16)
            gu[0] = gate
            gu[1] = upper
            for which in range(n_ff):
                @pl.when(chunk == which)
                def _():
                    w_next(w_base + base_g + 2 * which)
                    w_next(w_base + base_g + 2 * which + 1)
            return carry

        lax.fori_loop(0, n_ff, gate_up, 0)
        silu_mul(n_ff - 1)

        last = layer + 1 == layers

        def down(tile, carry):
            total = None
            for deep in range(n_deep):
                slot = lax.rem(w_base + base_d + tile * n_deep + deep, W_SLOTS)
                wait_slot(slot)
                part = jnp.dot(act_ref[:, deep * model:(deep + 1) * model], wbuf[slot], preferred_element_type=F32)
                total = part if total is None else total + part
            acc[:, at(tile * TILE, TILE, TILE)] = total
            exchange(2 * layer + 1, tile).start()
            for which in range(n_dn):
                @pl.when(tile == which)
                def _():
                    for deep in range(n_deep):
                        w_next(w_base + base_d + which * n_deep + deep)

            @pl.when(tile > 0)
            def _():
                settle(2 * layer + 1, tile - 1)
                if last:
                    send_group(tile - 1)
            return carry

        lax.fori_loop(0, n_dn, down, 0)
        settle(2 * layer + 1, n_dn - 1)
        if last:
            send_group(n_dn - 1)

        for dist in range(1, window // p_rows):
            @pl.when(chip + dist < chips)
            def _():
                halo(dist).wait_send()
        for dt, dc in peers:
            forward(dt, dc).wait_send()
            backward(dt, dc).wait_send()
        for dx in range(1, side // CORES):
            across(dx).wait()
        to_partner().start()
        if layer == 0:
            @pl.when(x_mine)
            def _():
                x_far.wait_send()

            y_far.wait_send()

    def hid_piece(grp, sub, c2):
        return hid_ref.at[pl.ds(sub * p_rows + c2 * half_p, half_p), pl.ds(grp * TILE, TILE)]

    def hid_pass(grp, sub, c2):
        return rc(hid_piece(grp, sub, c2), hid_piece(grp, sub, c2), hws.at[grp, sub * CORES + c2], fhr.at[grp, sub * CORES + c2], s_me, lax.rem(t_me + near[grp % 2], tp))

    def dec_pass(grp):
        piece = group(dec_ref, lax.rem(t_me + tp - near[grp % 2], tp) * d_rows, d_rows, d_rows, grp)
        return rc(piece, piece, dws.at[grp], fdr.at[grp, 2], s_me, lax.rem(t_me + near[grp % 2], tp))

    def origin(sub):
        return lax.rem(t_me + tp - (core * half_t + sub), tp)

    direct = [(sub, c2) for sub in range(half_t) for c2 in range(CORES)]
    for grp in range(n_groups):
        for sub, c2 in direct:
            gap = origin(sub)

            @pl.when((gap != 2) & jnp.logical_not((gap == 0) & (core == c2)))
            def _():
                hid_pass(grp, sub, c2).wait_recv()

            @pl.when(gap == near[grp % 2])
            def _():
                hid_pass(grp, sub, c2).start()

        dec_far(grp, near[grp % 2]).wait_recv()
        dec_pass(grp).start()
    for grp in range(n_groups):
        dec_far(grp, near[1 - grp % 2]).wait_recv()
        dec_far(grp, 2).wait_recv()
        for sub, c2 in direct:
            gap = origin(sub)

            @pl.when(gap == 2)
            def _():
                hid_pass(grp, sub, c2).wait_recv()

            @pl.when(gap == near[grp % 2])
            def _():
                hid_pass(grp, sub, c2).wait_send()

        dec_pass(grp).wait_send()
        for dt in near:
            hid_far(grp, dt).wait_send()
            dec_far(grp, dt).wait_send()

        @pl.when(own_hid)
        def _():
            hid_local(grp).wait()

        @pl.when(jnp.logical_not(own_hid))
        def _():
            hid_far(grp, 0).wait_send()

        dec_local(grp).wait()
    for handed in partners:
        handed().wait()


def finish_kernel(req_ref, dest_ref, len_ref, knv_ref, hid_ref, dec_ref, inst_ref, k_ref, v_ref,
                  hout_ref, dout_ref, kp_ref, vp_ref, kout_ref, vout_ref, kv_buf, ibuf, hbuf, dbuf, ksem, isem, hsem):
    layers, tp, slots, wide, batch = knv_ref.shape
    head_dim = wide // 2
    t_len = kv_buf.shape[5]
    win = ibuf.shape[2]
    max_req = kp_ref.shape[2]
    s_me = lax.axis_index('side')
    chunks = [(layer, part) for layer in range(layers) for part in range(tp)]

    def caches(num, which, out):
        layer, part = chunks[num]
        far = ((k_ref, v_ref), (kout_ref, vout_ref))[out][which].at[layer, pl.ds(part * batch, batch)]
        near = kv_buf.at[num, which]
        return pltpu.make_async_copy(near, far, ksem.at[num, which, 1]) if out else pltpu.make_async_copy(far, near, ksem.at[num, which, 0])

    cum = req_ref[0] * 0
    start = cum
    length = cum
    for req in range(req_ref.shape[0]):
        start = jnp.where(dest_ref[req] == s_me, cum, start)
        length = jnp.where(dest_ref[req] == s_me, req_ref[req], length)
        cum = cum + req_ref[req]
    blk = jnp.minimum((start // 64) * 64, inst_ref.shape[2] - win)
    grabs = [pltpu.make_async_copy(inst_ref.at[layer, :, pl.ds(pl.multiple_of(blk, 64), win), :], ibuf.at[layer], isem.at[layer]) for layer in range(layers)]
    for num in range(len(chunks)):
        for which in range(2):
            caches(num, which, 0).start()
        if num == 1:
            for one in grabs:
                one.start()
    h_in = [pltpu.make_async_copy(hid_ref, hbuf, hsem.at[0]), pltpu.make_async_copy(dec_ref, dbuf, hsem.at[1])]
    h_out = [pltpu.make_async_copy(hbuf, hout_ref, hsem.at[2]), pltpu.make_async_copy(dbuf, dout_ref, hsem.at[3])]
    for one in h_in:
        one.start()
    row = blk + lax.broadcasted_iota(jnp.int32, (win, max_req), 0)
    want = lax.broadcasted_iota(jnp.int32, (win, max_req), 1)
    pick = jnp.where((row - start == want) & (want < length), 1.0, 0.0).astype(BF16)
    t_iota = lax.broadcasted_iota(jnp.int32, (batch, t_len), 1)
    b_iota = lax.broadcasted_iota(jnp.int32, (batch, t_len), 0)
    for num, (layer, part) in enumerate(chunks):
        spots = [t_iota == len_ref[part * batch + b] for b in range(batch)]
        put = jnp.concatenate([jnp.where(spots[b] & (b_iota == b), 1.0, 0.0).astype(BF16) for b in range(batch)], axis=1)
        news = [jnp.dot(knv_ref[layer, part, slot], put, preferred_element_type=F32) for slot in range(slots)]
        for which in range(2):
            caches(num, which, 0).wait()
        for slot in range(slots):
            for b in range(batch):
                here = jnp.where(spots[b], 1.0, 0.0)
                here = jnp.concatenate([here] * (head_dim // batch), axis=0).astype(BF16) > 0
                new = news[slot][:, b * t_len:(b + 1) * t_len].astype(BF16)
                for which in range(2):
                    kv_buf[num, which, b, slot] = jnp.where(here, new[which * head_dim:(which + 1) * head_dim], kv_buf[num, which, b, slot])
        for which in range(2):
            caches(num, which, 1).start()
        if part == 1:
            grabs[layer].wait()
            for slot in range(slots):
                both = lax.dot_general(ibuf[layer, slot], pick, (((0,), (0,)), ((), ())), preferred_element_type=F32).astype(BF16)
                kp_ref[layer, slot * head_dim:(slot + 1) * head_dim, :] = both[:head_dim]
                vp_ref[layer, slot * head_dim:(slot + 1) * head_dim, :] = both[head_dim:]
    for one in h_in:
        one.wait()
    for one in h_out:
        one.start()
    for num in range(len(chunks)):
        for which in range(2):
            caches(num, which, 1).wait()
    for one in h_out:
        one.wait()


def solution(mesh):
    tp = mesh.shape['tp']
    side = mesh.shape['side']
    rows_spec = P(('pair', 'side'), None)
    batch_spec = P(('pair', 'side'), None, None)
    cache_spec = P(('pair', 'side'), None, None, None, 'tp', None)
    prompt_spec = P(('pair', 'side'), None, None, 'tp', None)

    def local_step(x_loc, req_len, dest, w_qkv, w_out, w_gate, w_up, w_down, y_loc, kc_loc, vc_loc, clen_loc):
        layers = w_qkv.shape[0]
        head_dim = kc_loc.shape[-1]
        slots = kc_loc.shape[-2]
        t_len = kc_loc.shape[3]
        batch = y_loc.shape[1]
        kv_heads = slots * tp
        rep = w_out.shape[1] // head_dim // kv_heads
        model = x_loc.shape[1]
        prompt_rows = x_loc.shape[0]
        seq_len = prompt_rows * side
        max_req = 2 * prompt_rows - prompt_rows // 4
        p_rows = prompt_rows * CORES // tp
        d_rows = batch // tp
        rows = p_rows + CORES * d_rows
        q_loc = w_out.shape[1] // CORES
        kv_loc = kv_heads // CORES * head_dim
        heads = kv_heads // CORES
        window = -(-(max_req - 1) // p_rows) * p_rows + p_rows
        group_w = rep * head_dim

        lengths = clen_loc[0]
        kc = jnp.transpose(kc_loc[0], (0, 1, 3, 4, 2))
        vc = jnp.transpose(vc_loc[0], (0, 1, 3, 4, 2))
        ff_loc = w_gate.shape[2] // CORES
        groups = model // TILE

        dma = pltpu.SemaphoreType.DMA
        n_peer = tp * CORES
        hid, dec, inst, knv = pl.pallas_call(
            functools.partial(mega_kernel, (side, tp, layers, head_dim, rep, slots)),
            out_shape=[jax.ShapeDtypeStruct((prompt_rows, model), BF16), jax.ShapeDtypeStruct((batch, model), BF16),
                       jax.ShapeDtypeStruct((layers, CORES, seq_len, 2 * head_dim), BF16),
                       jax.ShapeDtypeStruct((layers, tp, CORES, 2 * head_dim, d_rows), BF16)],
            in_specs=[SMEM, VMEM, ANY, ANY, ANY, ANY, ANY, ANY, ANY, ANY, ANY],
            out_specs=[ANY, ANY, ANY, VMEM],
            scratch_shapes=[
                pltpu.VMEM((W_SLOTS, model, TILE), BF16),
                pltpu.VMEM((rows, model), BF16),
                pltpu.VMEM((rows, model), F32),
                pltpu.VMEM((rows, model), BF16),
                pltpu.VMEM((rows, model), F32),
                pltpu.VMEM((2 * layers, rows, model), F32),
                pltpu.VMEM((rows, q_loc + 2 * kv_loc), BF16),
                pltpu.VMEM((layers, window, 2 * kv_loc), BF16),
                pltpu.VMEM((layers, CORES, heads, d_rows, group_w + 2 * head_dim), BF16),
                pltpu.VMEM((layers, tp, CORES, d_rows, group_w + 2 * head_dim), BF16),
                pltpu.VMEM((layers, n_peer, d_rows, group_w), BF16),
                pltpu.VMEM((layers, rows, q_loc), BF16),
                pltpu.VMEM((layers, heads, p_rows, 2 * head_dim), BF16),
                pltpu.VMEM((batch, slots, head_dim, t_len), BF16),
                pltpu.VMEM((batch, slots, head_dim, t_len), BF16),
                pltpu.VMEM((rows, ff_loc), BF16),
                pltpu.VMEM((2, rows, TILE), BF16),
                pltpu.VMEM((p_rows, window), F32),
                pltpu.VMEM((p_rows, 2 * head_dim), F32), pltpu.VMEM((p_rows, 2 * head_dim), F32),
                pltpu.VMEM((n_peer * d_rows, 2 * head_dim), F32), pltpu.VMEM((n_peer * d_rows, 2 * head_dim), F32),
                pltpu.VMEM((n_peer * rep * d_rows, 1), jnp.int32),
                dma((W_SLOTS, 2)), dma((6,)), dma((2,)),
                dma((2 * layers, groups)), dma((2 * layers, groups)),
                dma((layers, 4)), dma((layers, 4)),
                dma((layers, n_peer)), dma((layers, n_peer)),
                dma((layers, n_peer)), dma((layers, n_peer)),
                dma((layers, tp)), dma((layers, tp)), dma((layers, side // CORES)), dma((layers, side // CORES)), dma((layers,)), dma((layers,)), dma((layers,)),
                dma((groups, tp)), dma((groups, tp)), dma((groups, tp)), dma((groups, tp)), dma((groups, tp)), dma((groups,)), dma((2, groups)),
            ],
            compiler_params=pltpu.CompilerParams(collective_id=0, has_side_effects=True, vmem_limit_bytes=67043328),
            name="mega",
        )(req_len, clen_loc, x_loc, y_loc[0], kc, vc, w_qkv, w_out, w_gate, w_up, w_down)

        win = 512
        hid, dec, kp, vp, k_out, v_out = pl.pallas_call(
            finish_kernel,
            out_shape=[jax.ShapeDtypeStruct(hid.shape, BF16), jax.ShapeDtypeStruct(dec.shape, BF16)]
            + [jax.ShapeDtypeStruct((layers, slots * head_dim, max_req), BF16)] * 2 + [jax.ShapeDtypeStruct(kc.shape, BF16)] * 2,
            in_specs=[SMEM, SMEM, SMEM, VMEM, ANY, ANY, ANY, ANY, ANY],
            out_specs=[ANY, ANY, VMEM, VMEM, ANY, ANY],
            scratch_shapes=[
                pltpu.VMEM((layers * tp, 2, d_rows, slots, head_dim, t_len), BF16),
                pltpu.VMEM((layers, slots, win, 2 * head_dim), BF16),
                pltpu.VMEM(hid.shape, BF16), pltpu.VMEM(dec.shape, BF16),
                dma((layers * tp, 2, 2)), dma((layers,)), dma((4,)),
            ],
            compiler_params=pltpu.CompilerParams(vmem_limit_bytes=67043328),
            name="finish",
        )(req_len, dest, lengths, knv, hid, dec, inst, kc, vc)

        def cache_back(arr):
            return jnp.transpose(arr, (0, 1, 4, 2, 3))[None]

        def prompt_back(arr):
            return jnp.transpose(arr.reshape(layers, slots, head_dim, max_req), (0, 3, 1, 2))[None]

        return hid, dec[None], prompt_back(kp), prompt_back(vp), cache_back(k_out), cache_back(v_out)

    return jax.shard_map(local_step, mesh=mesh,
                         in_specs=(rows_spec, P('pair'), P('pair'), P(), P(), P(), P(), P(), batch_spec, cache_spec, cache_spec, rows_spec),
                         out_specs=(rows_spec, batch_spec, prompt_spec, prompt_spec, cache_spec, cache_spec),
                         check_vma=False)
```

```python
import functools
import math

import jax
import jax.numpy as jnp
from jax import lax
from jax.experimental import pallas as pl
from jax.experimental.pallas import tpu as pltpu
from jax.sharding import PartitionSpec as P

ROPE_BASE = 10000.0
NORM_EPS = 1e-5
BF16 = jnp.bfloat16
F32 = jnp.float32
TILE = 512
W_SLOTS = 18
CORES = 2
HALVES = 1
ANY = pl.BlockSpec(memory_space=pl.ANY)
VMEM = pl.BlockSpec(memory_space=pltpu.VMEM)
SMEM = pl.BlockSpec(memory_space=pltpu.SMEM)
MESH = pl.DeviceIdType.MESH
NT = (((1,), (1,)), ((), ()))


def rms(wide):
    return (wide * lax.rsqrt(jnp.mean(wide * wide, axis=-1, keepdims=True) + NORM_EPS)).astype(BF16)


def rope_tile(vals, cos, sin, head_dim):
    wide = vals.astype(F32)
    width = wide.shape[1]
    half = head_dim // 2
    lane = lax.broadcasted_iota(jnp.int32, wide.shape, 1)
    other = jnp.where(lax.rem(lane, head_dim) < half, pltpu.roll(wide, width - half, 1), pltpu.roll(wide, half, 1))
    reps = width // cos.shape[1]
    return (wide * jnp.concatenate([cos] * reps, axis=1) + other * jnp.concatenate([sin] * reps, axis=1)).astype(BF16)


def to_column(row, count, owner):
    n = row.shape[1]
    j = lax.broadcasted_iota(jnp.int32, (count, n), 0)
    return jnp.sum(jnp.where(lax.broadcasted_iota(jnp.int32, (count, n), 1) == owner(j), row.astype(F32), 0.0), axis=-1, keepdims=True)


def mega_kernel(cfg, req_ref, clen_ref, x_ref, y_ref, kc_ref, vc_ref, wq_ref, wo_ref, wg_ref, wu_ref, wd_ref,
                hid_ref, dec_ref, inst_ref, knv_ref,
                wbuf, hin, h_ref, norm_ref, acc, xch, qkv, kvwin, dsend, rdec, cback, ctx, isend, kbuf, vbuf, act_ref, gu, mask_ref, cos_ref, sin_ref, cosd_ref, sind_ref, len_ref,
                wsem, insem, csem, xsend, xrecv, kvs, kvr, kfs, dss, dsr, cbs, cbr, i1s, i1r, i2s, i2r, i3s, i3r, ilo, fhs, fhr, fds, fdr, hws, dws, flo):
    side, tp, layers, head_dim, rep, slots = cfg
    s_me = lax.axis_index('side')
    t_me = lax.axis_index('tp')
    core = lax.rem(s_me, CORES)
    col = s_me // CORES
    chip = col * tp + t_me
    chips = side // CORES * tp
    partner = s_me + 1 - 2 * core
    model = h_ref.shape[1]
    rows = h_ref.shape[0]
    p_rows = mask_ref.shape[0]
    d_rows = (rows - p_rows) // CORES
    half_p = p_rows // 2
    window = kvwin.shape[1]
    q_loc = ctx.shape[2]
    group_w = rep * head_dim
    heads = q_loc // group_w
    kv_loc = heads * head_dim
    q_all = wo_ref.shape[1]
    kv_all = (wq_ref.shape[2] - q_all) // 2
    ff_loc = wg_ref.shape[2] // CORES
    n_ff = ff_loc // TILE
    n_q = q_loc // TILE
    n_o = model * q_loc // (TILE * model)
    n_deep = ff_loc // model
    n_dn = model // TILE
    base_o = 1 + n_q
    base_g = base_o + n_o
    base_d = base_g + 2 * n_ff
    n_w = base_d + n_dn * n_deep

    def rc(src, dst, ssem, rsem, s_dev, t_dev):
        return pltpu.make_async_remote_copy(src_ref=src, dst_ref=dst, send_sem=ssem, recv_sem=rsem,
                                            device_id={'side': s_dev, 'tp': t_dev}, device_id_type=MESH)

    def at(base, size, unit):
        return pl.ds(pl.multiple_of(base, unit), size)

    def w_copies(idx):
        layer, pos = divmod(idx, n_w)
        slot = idx % W_SLOTS
        dst = wbuf.at[slot]
        if pos == 0:
            return [pltpu.make_async_copy(wq_ref.at[layer, :, at(q_all + core * kv_loc, kv_loc, 128)], dst.at[:, pl.ds(0, kv_loc)], wsem.at[slot, 0]),
                    pltpu.make_async_copy(wq_ref.at[layer, :, at(q_all + kv_all + core * kv_loc, kv_loc, 128)], dst.at[:, pl.ds(kv_loc, kv_loc)], wsem.at[slot, 1])]
        if pos < base_o:
            return [pltpu.make_async_copy(wq_ref.at[layer, :, at(core * q_loc + (pos - 1) * TILE, TILE, TILE)], dst, wsem.at[slot, 0])]
        if pos < base_g:
            pos -= base_o
            return [pltpu.make_async_copy(wo_ref.at[layer, at(core * q_loc, q_loc, q_loc), pl.ds((2 * pos + part) * TILE, TILE)], dst.at[pl.ds(part * q_loc, q_loc), :], wsem.at[slot, part]) for part in range(2)]
        if pos < base_d:
            pos -= base_g
            src = (wg_ref, wu_ref)[pos % 2]
            return [pltpu.make_async_copy(src.at[layer, :, at(core * ff_loc + (pos // 2) * TILE, TILE, TILE)], dst, wsem.at[slot, 0])]
        pos -= base_d
        return [pltpu.make_async_copy(wd_ref.at[layer, at(core * ff_loc + pos % n_deep * model, model, model), pl.ds(pos // n_deep * TILE, TILE)], dst, wsem.at[slot, 0])]

    def start_all(copies):
        for one in copies:
            one.start()

    def wait_all(copies):
        for one in copies:
            one.wait()

    def w_next(idx):
        if idx + W_SLOTS < layers * n_w:
            start_all(w_copies(idx + W_SLOTS))

    def cache_copies(layer):
        return [pltpu.make_async_copy(kc_ref.at[layer], kbuf, csem.at[0]), pltpu.make_async_copy(vc_ref.at[layer], vbuf, csem.at[1])]

    x_mine = core == t_me // (tp // CORES)
    x_src = x_ref.at[at(lax.rem(t_me, tp // CORES) * p_rows, p_rows, p_rows), :]
    x_dst = hin.at[pl.ds(0, p_rows), :]
    y_src = y_ref.at[at(t_me * d_rows, d_rows, d_rows), :]
    y_dst = hin.at[at(p_rows + core * d_rows, d_rows, d_rows), :]
    x_local = pltpu.make_async_copy(x_src, x_dst, insem.at[0])
    y_local = pltpu.make_async_copy(y_src, y_dst, insem.at[1])
    x_far = rc(x_dst, x_dst, insem.at[2], insem.at[3], partner, t_me)
    y_far = rc(y_dst, y_dst, insem.at[4], insem.at[5], partner, t_me)

    @pl.when(x_mine)
    def _():
        x_local.start()

    y_local.start()
    start_all(w_copies(0))

    barrier = pltpu.get_barrier_semaphore()
    for ds in range(side):
        for dt in range(tp):
            if ds or dt:
                pl.semaphore_signal(barrier, inc=1, device_id={'side': lax.rem(s_me + ds, side), 'tp': lax.rem(t_me + dt, tp)}, device_id_type=MESH)

    for idx in range(1, W_SLOTS):
        start_all(w_copies(idx))
        if idx == 2:
            start_all(cache_copies(0))

    for layer in range(layers):
        for dist in range(1, window // p_rows):
            @pl.when(chip < dist)
            def _():
                hi = window - p_rows * dist
                kvwin[layer, hi - p_rows:hi, :] = jnp.zeros((p_rows, kvwin.shape[2]), BF16)

    gu[...] = jnp.zeros_like(gu)

    lane = lax.broadcasted_iota(jnp.int32, (p_rows, 2 * head_dim), 1)
    freq = jnp.exp((lane & (head_dim // 2 - 1)).astype(F32) * (-math.log(ROPE_BASE) / (head_dim // 2)))
    sign = jnp.where((lane & (head_dim - 1)) < head_dim // 2, -1.0, 1.0)
    q_row = chip * p_rows + lax.broadcasted_iota(jnp.int32, (p_rows, 2 * head_dim), 0)
    seg = jnp.zeros_like(q_row)
    end = req_ref[0] * 0
    for req in range(side):
        end = end + req_ref[req]
        seg = seg + jnp.where(q_row >= end, req_ref[req], 0)
    angles = (q_row - seg).astype(F32) * freq
    cos_ref[...] = jnp.cos(angles)
    sin_ref[...] = jnp.sin(angles) * sign
    dec_pos = to_column(clen_ref[...], tp * CORES * d_rows, lambda j: (j // (CORES * d_rows)) * d_rows + (j & (d_rows - 1)))
    angles = dec_pos * freq
    cosd_ref[...] = jnp.cos(angles)
    sind_ref[...] = jnp.sin(angles) * sign
    len_ref[...] = to_column(clen_ref[...], tp * CORES * rep * d_rows, lambda j: (j // (CORES * rep * d_rows)) * d_rows + (j & (d_rows - 1))).astype(jnp.int32)
    for piece in range(window // (2 * head_dim)):
        key_row = (chip + 1) * p_rows - window + piece * 2 * head_dim + lane
        mask_ref[:, piece * 2 * head_dim:(piece + 1) * 2 * head_dim] = jnp.where((key_row <= q_row) & (key_row >= seg), 1.0, 0.0)

    pl.semaphore_wait(barrier, side * tp - 1)

    y_local.wait()
    y_far.start()

    @pl.when(x_mine)
    def _():
        x_local.wait()
        x_far.start()

    @pl.when(jnp.logical_not(x_mine))
    def _():
        x_far.wait_recv()

    y_far.wait_recv()
    h_ref[...] = hin[...].astype(F32)

    diag = (lax.broadcasted_iota(jnp.int32, (d_rows, d_rows * head_dim), 1) // head_dim) == lax.broadcasted_iota(jnp.int32, (d_rows, d_rows * head_dim), 0)
    scale = head_dim ** -0.5
    n_peer = tp * CORES

    def exchange(idx, grp):
        sl = at(grp * TILE, TILE, TILE)
        return rc(acc.at[:, sl], xch.at[idx, :, sl], xsend.at[idx, grp], xrecv.at[idx, grp], partner, t_me)

    def settle(idx, grp):
        exchange(idx, grp).wait()
        sl = at(grp * TILE, TILE, TILE)
        h_ref[:, sl] = (h_ref[:, sl] + (acc[:, sl] + xch[idx, :, sl]).astype(BF16).astype(F32)).astype(BF16).astype(F32)

    half_t = tp // CORES
    own_hid = core == t_me // half_t
    piece_me = lax.rem(t_me, half_t) * CORES + core
    n_groups = model // TILE

    def group(ref, base, size, unit, grp):
        return ref.at[at(base, size, unit), at(grp * TILE, TILE, TILE)]

    def hid_src(grp):
        return group(hin, core * half_p, half_p, half_p, grp)

    def hid_dst(grp):
        return group(hid_ref, lax.rem(t_me, half_t) * p_rows + core * half_p, half_p, half_p, grp)

    def hid_local(grp):
        return pltpu.make_async_copy(hid_src(grp), hid_dst(grp), flo.at[0, grp])

    def hid_far(grp, dt):
        return rc(hid_src(grp), hid_dst(grp), fhs.at[grp, dt], fhr.at[grp, piece_me], col * CORES + t_me // half_t, lax.rem(t_me + dt, tp))

    def dec_src(grp):
        return group(hin, p_rows + core * d_rows, d_rows, d_rows, grp)

    def dec_dst(grp):
        return group(dec_ref, t_me * d_rows, d_rows, d_rows, grp)

    def dec_local(grp):
        return pltpu.make_async_copy(dec_src(grp), dec_dst(grp), flo.at[1, grp])

    def dec_far(grp, dt):
        return rc(dec_src(grp), dec_dst(grp), fds.at[grp, dt], fdr.at[grp, dt], s_me, lax.rem(t_me + dt, tp))

    near = (1, tp - 1)

    def send_group(grp):
        sl = at(grp * TILE, TILE, TILE)
        hin[:, sl] = h_ref[:, sl].astype(BF16)
        for dt in near:
            hid_far(grp, dt).start()
            dec_far(grp, dt).start()

        @pl.when(own_hid)
        def _():
            hid_local(grp).start()

        @pl.when(jnp.logical_not(own_hid))
        def _():
            hid_far(grp, 0).start()

        dec_local(grp).start()

    partners = []
    for layer in range(layers):
        w_base = layer * n_w
        norm_ref[...] = rms(h_ref[...])
        cos = cos_ref[...]
        sin = sin_ref[...]

        wait_all(w_copies(w_base))
        out = jnp.dot(norm_ref[...], wbuf[(w_base) % W_SLOTS], preferred_element_type=F32).astype(BF16)
        w_next(w_base)
        qkv[:, q_loc:] = out
        kvwin[layer, window - p_rows:, 0:kv_loc] = rope_tile(out[:p_rows, :kv_loc], cos, sin, head_dim)
        kvwin[layer, window - p_rows:, kv_loc:] = out[:p_rows, kv_loc:]

        def block(dist):
            hi = window - p_rows * dist
            return kvwin.at[layer, pl.ds(hi - p_rows, p_rows), :]

        def halo(dist):
            target = chip + dist
            return rc(block(0), block(dist), kvs.at[layer, dist - 1], kvr.at[layer, dist - 1], CORES * (target // tp) + core, lax.rem(target, tp))

        def goes(dist):
            return col + 1 < side // CORES if dist == tp else t_me + dist < tp

        def hand_on(place):
            dist = tp + place - t_me
            hi = window - p_rows * dist
            dst = kvwin.at[layer, at(hi - p_rows, p_rows, p_rows), :]
            return rc(block(tp), dst, kfs.at[layer, place], kvr.at[layer, dist - 1], s_me, place)

        def hands_on(place):
            return (col > 0) & (place < t_me)

        for dist in (tp, 1):
            @pl.when(goes(dist))
            def _():
                halo(dist).start()

        for tile in range(n_q):
            idx = w_base + 1 + tile
            wait_all(w_copies(idx))
            out = jnp.dot(norm_ref[...], wbuf[idx % W_SLOTS], preferred_element_type=F32).astype(BF16)
            w_next(idx)
            sl = slice(tile * TILE, (tile + 1) * TILE)
            qkv[:p_rows, sl] = rope_tile(out[:p_rows], cos, sin, head_dim)
            qkv[p_rows:, sl] = out[p_rows:]

        for sub in range(CORES):
            for head in range(heads):
                r0 = p_rows + sub * d_rows
                kk = qkv[r0:r0 + d_rows, q_loc + head * head_dim:q_loc + (head + 1) * head_dim]
                vv = qkv[r0:r0 + d_rows, q_loc + kv_loc + head * head_dim:q_loc + kv_loc + (head + 1) * head_dim]
                dsend[layer, sub, head, :, 0:group_w] = qkv[r0:r0 + d_rows, head * group_w:(head + 1) * group_w]
                dsend[layer, sub, head, :, group_w:] = jnp.concatenate([kk, vv], axis=1)

        def forward(dt, dc):
            s2 = lax.rem(core + dc, CORES)
            t2 = lax.rem(t_me + dt, tp)
            return rc(dsend.at[layer, s2, t2], rdec.at[layer, t_me, core], dss.at[layer, dt * CORES + dc], dsr.at[layer, dt * CORES + dc], col * CORES + s2, t2)

        peers = [(dt, dc) for dt in range(tp) for dc in range(CORES) if dt or dc]
        for dt, dc in peers:
            forward(dt, dc).start()
        rdec[layer, t_me, core] = dsend[layer, core, t_me]
        for dist in range(2, tp):
            @pl.when(goes(dist))
            def _():
                halo(dist).start()

        @pl.when(col > 0)
        def _():
            halo(tp).wait_recv()

        for place in range(tp - 1):
            @pl.when(hands_on(place))
            def _():
                hand_on(place).start()

        def backward(dt, dc):
            t2 = lax.rem(t_me + tp - dt, tp)
            c2 = lax.rem(core + dc, CORES)
            dst = ctx.at[layer, at(p_rows + core * d_rows, d_rows, d_rows), at(t_me * group_w, group_w, group_w)]
            return rc(cback.at[layer, t2 * CORES + c2], dst, cbs.at[layer, dt * CORES + dc], cbr.at[layer, dt * CORES + dc], col * CORES + c2, t2)

        wait_all(cache_copies(layer))
        for dt, dc in peers:
            forward(dt, dc).wait_recv()
        raw = jnp.concatenate([rdec[layer, p // CORES, p % CORES] for p in range(n_peer)], axis=0)
        roped = rope_tile(raw, cosd_ref[...], sind_ref[...], head_dim)
        q_wide = roped[:, :group_w].astype(F32) * scale
        k_new = roped[:, group_w:group_w + head_dim].astype(F32)
        v_new = raw[:, group_w + head_dim:].astype(F32)
        eye = jnp.where(lax.broadcasted_iota(jnp.int32, (d_rows, d_rows), 0) == lax.broadcasted_iota(jnp.int32, (d_rows, d_rows), 1), 1.0, 0.0).astype(BF16)
        both = jnp.concatenate([k_new, v_new], axis=1).astype(BF16)
        scores = []
        fresh = []
        for p in range(n_peer):
            rs = slice(p * d_rows, (p + 1) * d_rows)
            knv_ref[layer, p // CORES, p % CORES] = lax.dot_general(both[rs], eye, (((0,), (0,)), ((), ())), preferred_element_type=F32).astype(BF16)
            q_parts = [q_wide[rs, r * head_dim:(r + 1) * head_dim] for r in range(rep)]
            pairs = [jnp.concatenate([part, part], axis=1) for part in q_parts]
            lhs = jnp.concatenate([jnp.where(diag, jnp.concatenate([pair] * (d_rows // 2), axis=1), 0.0) for pair in pairs], axis=0).astype(BF16)
            y2 = p // CORES
            k_part = kbuf[y2 * d_rows:(y2 + 1) * d_rows, p % CORES].reshape(d_rows * head_dim, kbuf.shape[3])
            scores.append(jnp.dot(lhs, k_part, preferred_element_type=F32))
            fresh.append(jnp.concatenate(q_parts, axis=0) * jnp.concatenate([k_new[rs]] * rep, axis=0))
        scores = jnp.concatenate(scores, axis=0)
        s_new = jnp.sum(jnp.concatenate(fresh, axis=0), axis=-1, keepdims=True)
        where_new = len_ref[...]
        pos = lax.broadcasted_iota(jnp.int32, scores.shape, 1)
        scores = jnp.where(pos < where_new, scores, -1e30)
        scores = jnp.where(pos == where_new, s_new, scores)
        scores = jnp.exp(scores - jnp.max(scores, axis=-1, keepdims=True))
        prob = (scores * (1.0 / jnp.sum(scores, axis=-1, keepdims=True))).astype(BF16).astype(F32)
        p_new = jnp.sum(jnp.where(pos == where_new, prob, 0.0), axis=-1, keepdims=True)
        p_old = jnp.where(pos == where_new, 0.0, prob).astype(BF16)
        grp_rows = rep * d_rows
        for p in range(n_peer):
            y2 = p // CORES
            gs = slice(p * grp_rows, (p + 1) * grp_rows)
            v_part = vbuf[y2 * d_rows:(y2 + 1) * d_rows, p % CORES].reshape(d_rows * head_dim, vbuf.shape[3])
            full = lax.dot_general(p_old[gs], v_part, NT, preferred_element_type=F32)
            full = jnp.where(jnp.concatenate([diag] * rep, axis=0), full, 0.0)
            fold = full[:, 0:128]
            for piece in range(1, full.shape[1] // 128):
                fold = fold + full[:, piece * 128:(piece + 1) * 128]
            got = fold[:, :head_dim] + fold[:, head_dim:] + p_new[gs] * jnp.concatenate([v_new[p * d_rows:(p + 1) * d_rows]] * rep, axis=0)
            cback[layer, p] = jnp.concatenate([got[r * d_rows:(r + 1) * d_rows] for r in range(rep)], axis=1).astype(BF16)
        for dt, dc in peers:
            backward(dt, dc).start()
        ctx[layer, at(p_rows + core * d_rows, d_rows, d_rows), at(t_me * group_w, group_w, group_w)] = cback[layer, t_me * CORES + core]
        if layer + 1 < layers:
            start_all(cache_copies(layer + 1))

        for dist in range(1, tp):
            @pl.when(chip >= dist)
            def _():
                halo(dist).wait_recv()

        allowed = mask_ref[...] > 0.5
        for head in range(heads):
            k_head = kvwin[layer, :, head * head_dim:(head + 1) * head_dim]
            v_head = kvwin[layer, :, kv_loc + head * head_dim:kv_loc + (head + 1) * head_dim]
            q0 = head * group_w
            q_part = jnp.concatenate([qkv[:p_rows, q0 + sub * head_dim:q0 + (sub + 1) * head_dim] for sub in range(rep)], axis=0)
            q_part = (q_part.astype(F32) * scale).astype(BF16)
            scores = lax.dot_general(q_part, k_head, NT, preferred_element_type=F32).reshape(rep, p_rows, window)
            scores = jnp.where(allowed[None], scores, -1e30)
            scores = jnp.exp(scores - jnp.max(scores, axis=-1, keepdims=True))
            prob = (scores * (1.0 / jnp.sum(scores, axis=-1, keepdims=True))).astype(BF16).reshape(rep * p_rows, window)
            got = jnp.dot(prob, v_head, preferred_element_type=F32).astype(BF16)
            outs = [got[sub * p_rows:(sub + 1) * p_rows] for sub in range(rep)]
            ctx[layer, 0:p_rows, q0:q0 + group_w] = jnp.concatenate(outs, axis=1)
            isend[layer, head] = jnp.concatenate([k_head[window - p_rows:], v_head[window - p_rows:]], axis=1)

        def spread(dt):
            t2 = lax.rem(t_me + dt, tp)
            return rc(isend.at[layer, t2], inst_ref.at[layer, core, at(chip * p_rows, p_rows, p_rows), :], i1s.at[layer, dt], i1r.at[layer, dt], s_me, t2)

        def keep_own():
            return pltpu.make_async_copy(isend.at[layer, t_me], inst_ref.at[layer, core, at(chip * p_rows, p_rows, p_rows), :], ilo.at[layer])

        def across(dx):
            part = inst_ref.at[layer, core, at(col * tp * p_rows, tp * p_rows, tp * p_rows), :]
            return rc(part, part, i2s.at[layer, dx], i2r.at[layer, dx], lax.rem(col + dx, side // CORES) * CORES + core, t_me)

        def to_partner(layer=layer):
            return rc(inst_ref.at[layer, core], inst_ref.at[layer, core], i3s.at[layer], i3r.at[layer], partner, t_me)

        partners.append(to_partner)
        for dt in range(1, tp):
            spread(dt).start()
        keep_own().start()
        for dt, dc in peers:
            backward(dt, dc).wait_recv()

        for tile in range(n_o):
            idx = w_base + base_o + tile
            wait_all(w_copies(idx))
            for part in range(2):
                lo = (2 * tile + part) * TILE
                acc[:, lo:lo + TILE] = jnp.dot(ctx[layer], wbuf[idx % W_SLOTS, part * q_loc:(part + 1) * q_loc, :], preferred_element_type=F32)
                exchange(2 * layer, 2 * tile + part).start()
            w_next(idx)
        for grp in range(n_groups):
            settle(2 * layer, grp)
        norm_ref[...] = rms(h_ref[...])

        for dt in range(1, tp):
            spread(dt).wait()
        keep_own().wait()
        for dx in range(1, side // CORES):
            across(dx).start()

        def wait_slot(slot):
            pltpu.make_async_copy(wg_ref.at[layer, :, pl.ds(0, TILE)], wbuf.at[slot], wsem.at[slot, 0]).wait()

        def silu_mul(chunk):
            act_ref[:, at(chunk * TILE, TILE, TILE)] = (jax.nn.silu(gu[0].astype(F32)) * gu[1].astype(F32)).astype(BF16)

        def gate_up(chunk, carry):
            slot_g = lax.rem(w_base + base_g + 2 * chunk, W_SLOTS)
            slot_u = lax.rem(w_base + base_g + 2 * chunk + 1, W_SLOTS)
            wait_slot(slot_g)
            wait_slot(slot_u)
            gate = jnp.dot(norm_ref[...], wbuf[slot_g], preferred_element_type=F32).astype(BF16)
            silu_mul(jnp.maximum(chunk - 1, 0))
            upper = jnp.dot(norm_ref[...], wbuf[slot_u], preferred_element_type=F32).astype(BF16)
            gu[0] = gate
            gu[1] = upper
            for which in range(n_ff):
                @pl.when(chunk == which)
                def _():
                    w_next(w_base + base_g + 2 * which)
                    w_next(w_base + base_g + 2 * which + 1)
            return carry

        lax.fori_loop(0, n_ff, gate_up, 0)
        silu_mul(n_ff - 1)

        last = layer + 1 == layers

        def down(tile, carry):
            total = None
            for deep in range(n_deep):
                slot = lax.rem(w_base + base_d + tile * n_deep + deep, W_SLOTS)
                wait_slot(slot)
                part = jnp.dot(act_ref[:, deep * model:(deep + 1) * model], wbuf[slot], preferred_element_type=F32)
                total = part if total is None else total + part
            acc[:, at(tile * TILE, TILE, TILE)] = total
            exchange(2 * layer + 1, tile).start()
            for which in range(n_dn):
                @pl.when(tile == which)
                def _():
                    for deep in range(n_deep):
                        w_next(w_base + base_d + which * n_deep + deep)

            @pl.when(tile > 1)
            def _():
                settle(2 * layer + 1, tile - 2)
                if last:
                    send_group(tile - 2)
            return carry

        lax.fori_loop(0, n_dn, down, 0)
        for grp in range(n_dn - 2, n_dn):
            settle(2 * layer + 1, grp)
            if last:
                send_group(grp)

        for dist in range(1, tp + 1):
            @pl.when(goes(dist))
            def _():
                halo(dist).wait_send()
        for place in range(tp - 1):
            @pl.when(hands_on(place))
            def _():
                hand_on(place).wait_send()
        for dt, dc in peers:
            forward(dt, dc).wait_send()
            backward(dt, dc).wait_send()
        for dx in range(1, side // CORES):
            across(dx).wait()
        to_partner().start()
        if layer == 0:
            @pl.when(x_mine)
            def _():
                x_far.wait_send()

            y_far.wait_send()

    def hid_piece(grp, sub, c2):
        return hid_ref.at[pl.ds(sub * p_rows + c2 * half_p, half_p), pl.ds(grp * TILE, TILE)]

    def hid_pass(grp, sub, c2):
        return rc(hid_piece(grp, sub, c2), hid_piece(grp, sub, c2), hws.at[grp, sub * CORES + c2], fhr.at[grp, sub * CORES + c2], s_me, lax.rem(t_me + near[grp % 2], tp))

    def dec_pass(grp):
        piece = group(dec_ref, lax.rem(t_me + tp - near[grp % 2], tp) * d_rows, d_rows, d_rows, grp)
        return rc(piece, piece, dws.at[grp], fdr.at[grp, 2], s_me, lax.rem(t_me + near[grp % 2], tp))

    def origin(sub):
        return lax.rem(t_me + tp - (core * half_t + sub), tp)

    direct = [(sub, c2) for sub in range(half_t) for c2 in range(CORES)]
    for grp in range(n_groups):
        for sub, c2 in direct:
            gap = origin(sub)

            @pl.when((gap != 2) & jnp.logical_not((gap == 0) & (core == c2)))
            def _():
                hid_pass(grp, sub, c2).wait_recv()

            @pl.when(gap == near[grp % 2])
            def _():
                hid_pass(grp, sub, c2).start()

        dec_far(grp, near[grp % 2]).wait_recv()
        dec_pass(grp).start()
    for grp in range(n_groups):
        dec_far(grp, near[1 - grp % 2]).wait_recv()
        dec_far(grp, 2).wait_recv()
        for sub, c2 in direct:
            gap = origin(sub)

            @pl.when(gap == 2)
            def _():
                hid_pass(grp, sub, c2).wait_recv()

            @pl.when(gap == near[grp % 2])
            def _():
                hid_pass(grp, sub, c2).wait_send()

        dec_pass(grp).wait_send()
        for dt in near:
            hid_far(grp, dt).wait_send()
            dec_far(grp, dt).wait_send()

        @pl.when(own_hid)
        def _():
            hid_local(grp).wait()

        @pl.when(jnp.logical_not(own_hid))
        def _():
            hid_far(grp, 0).wait_send()

        dec_local(grp).wait()
    for handed in partners:
        handed().wait()


def finish_kernel(req_ref, dest_ref, len_ref, knv_hbm, hid_ref, dec_ref, inst_ref, k_ref, v_ref,
                  hout_ref, dout_ref, kp_out, vp_out, kout_ref, vout_ref, kv_buf, ibuf, hbuf, dbuf, knv_ref, kp_ref, vp_ref, ksem, isem, hsem):
    layers, tp, slots, wide, batch = knv_ref.shape
    head_dim = wide // 2
    t_len = kv_buf.shape[5]
    win = ibuf.shape[2]
    max_req = kp_ref.shape[2]
    s_me = lax.axis_index('side')
    total_b = tp * batch
    units = [(layer, which, half) for layer in range(layers) for half in range(HALVES) for which in range(2)]
    part_b = total_b // HALVES

    def caches(num, out):
        layer, which, half = units[num]
        rows = pl.ds(half * part_b, part_b)
        far = ((k_ref, v_ref), (kout_ref, vout_ref))[out][which].at[layer, rows]
        near = kv_buf.at[layer, which, rows]
        return pltpu.make_async_copy(near, far, ksem.at[num, 1]) if out else pltpu.make_async_copy(far, near, ksem.at[num, 0])

    cum = req_ref[0] * 0
    start = cum
    length = cum
    for req in range(req_ref.shape[0]):
        start = jnp.where(dest_ref[req] == s_me, cum, start)
        length = jnp.where(dest_ref[req] == s_me, req_ref[req], length)
        cum = cum + req_ref[req]
    blk = jnp.minimum((start // 64) * 64, inst_ref.shape[2] - win)
    grabs = [pltpu.make_async_copy(inst_ref.at[layer, :, pl.ds(pl.multiple_of(blk, 64), win), :], ibuf.at[layer], isem.at[layer]) for layer in range(layers)]
    knv_in = pltpu.make_async_copy(knv_hbm, knv_ref, hsem.at[4])
    prompt_out = [pltpu.make_async_copy(kp_ref, kp_out, hsem.at[5]), pltpu.make_async_copy(vp_ref, vp_out, hsem.at[6])]
    for one in grabs:
        one.start()
    knv_in.start()
    for num in range(len(units)):
        caches(num, 0).start()
    h_in = [pltpu.make_async_copy(hid_ref, hbuf, hsem.at[0]), pltpu.make_async_copy(dec_ref, dbuf, hsem.at[1])]
    h_out = [pltpu.make_async_copy(hbuf, hout_ref, hsem.at[2]), pltpu.make_async_copy(dbuf, dout_ref, hsem.at[3])]
    for one in h_in:
        one.start()
    row = blk + lax.broadcasted_iota(jnp.int32, (win, max_req), 0)
    want = lax.broadcasted_iota(jnp.int32, (win, max_req), 1)
    pick = jnp.where((row - start == want) & (want < length), 1.0, 0.0).astype(BF16)
    for lay in range(layers):
        grabs[lay].wait()
        for slot in range(slots):
            both = lax.dot_general(ibuf[lay, slot], pick, (((0,), (0,)), ((), ())), preferred_element_type=F32).astype(BF16)
            kp_ref[lay, slot * head_dim:(slot + 1) * head_dim, :] = both[:head_dim]
            vp_ref[lay, slot * head_dim:(slot + 1) * head_dim, :] = both[head_dim:]
    for one in prompt_out:
        one.start()
    knv_in.wait()
    t_iota = lax.broadcasted_iota(jnp.int32, (head_dim, t_len), 1)
    for num, (layer, which, half) in enumerate(units):
        caches(num, 0).wait()
        for b in range(half * part_b, (half + 1) * part_b):
            here = t_iota == len_ref[b]
            for slot in range(slots):
                new = knv_ref[layer, b // batch, slot, which * head_dim:(which + 1) * head_dim, b % batch:b % batch + 1].astype(F32)
                kv_buf[layer, which, b, slot] = jnp.where(here, new, kv_buf[layer, which, b, slot].astype(F32)).astype(BF16)
        caches(num, 1).start()
    for one in h_in:
        one.wait()
    for one in h_out:
        one.start()
    for num in range(len(units)):
        caches(num, 1).wait()
    for one in h_out + prompt_out:
        one.wait()


def solution(mesh):
    tp = mesh.shape['tp']
    side = mesh.shape['side']
    rows_spec = P(('pair', 'side'), None)
    batch_spec = P(('pair', 'side'), None, None)
    cache_spec = P(('pair', 'side'), None, None, None, 'tp', None)
    prompt_spec = P(('pair', 'side'), None, None, 'tp', None)

    def local_step(x_loc, req_len, dest, w_qkv, w_out, w_gate, w_up, w_down, y_loc, kc_loc, vc_loc, clen_loc):
        layers = w_qkv.shape[0]
        head_dim = kc_loc.shape[-1]
        slots = kc_loc.shape[-2]
        t_len = kc_loc.shape[3]
        batch = y_loc.shape[1]
        kv_heads = slots * tp
        rep = w_out.shape[1] // head_dim // kv_heads
        model = x_loc.shape[1]
        prompt_rows = x_loc.shape[0]
        seq_len = prompt_rows * side
        max_req = 2 * prompt_rows - prompt_rows // 4
        p_rows = prompt_rows * CORES // tp
        d_rows = batch // tp
        rows = p_rows + CORES * d_rows
        q_loc = w_out.shape[1] // CORES
        kv_loc = kv_heads // CORES * head_dim
        heads = kv_heads // CORES
        window = -(-(max_req - 1) // p_rows) * p_rows + p_rows
        assert window == (tp + 1) * p_rows
        group_w = rep * head_dim

        lengths = clen_loc[0]
        kc = jnp.transpose(kc_loc[0], (0, 1, 3, 4, 2))
        vc = jnp.transpose(vc_loc[0], (0, 1, 3, 4, 2))
        ff_loc = w_gate.shape[2] // CORES
        groups = model // TILE

        dma = pltpu.SemaphoreType.DMA
        n_peer = tp * CORES
        hid, dec, inst, knv = pl.pallas_call(
            functools.partial(mega_kernel, (side, tp, layers, head_dim, rep, slots)),
            out_shape=[jax.ShapeDtypeStruct((prompt_rows, model), BF16), jax.ShapeDtypeStruct((batch, model), BF16),
                       jax.ShapeDtypeStruct((layers, CORES, seq_len, 2 * head_dim), BF16),
                       jax.ShapeDtypeStruct((layers, tp, CORES, 2 * head_dim, d_rows), BF16)],
            in_specs=[SMEM, VMEM, ANY, ANY, ANY, ANY, ANY, ANY, ANY, ANY, ANY],
            out_specs=[ANY, ANY, ANY, VMEM],
            scratch_shapes=[
                pltpu.VMEM((W_SLOTS, model, TILE), BF16),
                pltpu.VMEM((rows, model), BF16),
                pltpu.VMEM((rows, model), F32),
                pltpu.VMEM((rows, model), BF16),
                pltpu.VMEM((rows, model), F32),
                pltpu.VMEM((2 * layers, rows, model), F32),
                pltpu.VMEM((rows, q_loc + 2 * kv_loc), BF16),
                pltpu.VMEM((layers, window, 2 * kv_loc), BF16),
                pltpu.VMEM((layers, CORES, heads, d_rows, group_w + 2 * head_dim), BF16),
                pltpu.VMEM((layers, tp, CORES, d_rows, group_w + 2 * head_dim), BF16),
                pltpu.VMEM((layers, n_peer, d_rows, group_w), BF16),
                pltpu.VMEM((layers, rows, q_loc), BF16),
                pltpu.VMEM((layers, heads, p_rows, 2 * head_dim), BF16),
                pltpu.VMEM((batch, slots, head_dim, t_len), BF16),
                pltpu.VMEM((batch, slots, head_dim, t_len), BF16),
                pltpu.VMEM((rows, ff_loc), BF16),
                pltpu.VMEM((2, rows, TILE), BF16),
                pltpu.VMEM((p_rows, window), F32),
                pltpu.VMEM((p_rows, 2 * head_dim), F32), pltpu.VMEM((p_rows, 2 * head_dim), F32),
                pltpu.VMEM((n_peer * d_rows, 2 * head_dim), F32), pltpu.VMEM((n_peer * d_rows, 2 * head_dim), F32),
                pltpu.VMEM((n_peer * rep * d_rows, 1), jnp.int32),
                dma((W_SLOTS, 2)), dma((6,)), dma((2,)),
                dma((2 * layers, groups)), dma((2 * layers, groups)),
                dma((layers, tp)), dma((layers, tp)), dma((layers, tp)),
                dma((layers, n_peer)), dma((layers, n_peer)),
                dma((layers, n_peer)), dma((layers, n_peer)),
                dma((layers, tp)), dma((layers, tp)), dma((layers, side // CORES)), dma((layers, side // CORES)), dma((layers,)), dma((layers,)), dma((layers,)),
                dma((groups, tp)), dma((groups, tp)), dma((groups, tp)), dma((groups, tp)), dma((groups, tp)), dma((groups,)), dma((2, groups)),
            ],
            compiler_params=pltpu.CompilerParams(collective_id=0, has_side_effects=True, vmem_limit_bytes=67043328),
            name="mega",
        )(req_len, clen_loc, x_loc, y_loc[0], kc, vc, w_qkv, w_out, w_gate, w_up, w_down)

        win = 512
        hid, dec, kp, vp, k_out, v_out = pl.pallas_call(
            finish_kernel,
            out_shape=[jax.ShapeDtypeStruct(hid.shape, BF16), jax.ShapeDtypeStruct(dec.shape, BF16)]
            + [jax.ShapeDtypeStruct((layers, slots * head_dim, max_req), BF16)] * 2 + [jax.ShapeDtypeStruct(kc.shape, BF16)] * 2,
            in_specs=[SMEM, SMEM, SMEM, ANY, ANY, ANY, ANY, ANY, ANY],
            out_specs=[ANY] * 6,
            scratch_shapes=[
                pltpu.VMEM((layers, 2, batch, slots, head_dim, t_len), BF16),
                pltpu.VMEM((layers, slots, win, 2 * head_dim), BF16),
                pltpu.VMEM(hid.shape, BF16), pltpu.VMEM(dec.shape, BF16), pltpu.VMEM(knv.shape, BF16),
                pltpu.VMEM((layers, slots * head_dim, max_req), BF16), pltpu.VMEM((layers, slots * head_dim, max_req), BF16),
                dma((2 * layers * HALVES, 2)), dma((layers,)), dma((7,)),
            ],
            compiler_params=pltpu.CompilerParams(vmem_limit_bytes=67043328),
            name="finish",
        )(req_len, dest, lengths, knv, hid, dec, inst, kc, vc)

        def cache_back(arr):
            return jnp.transpose(arr, (0, 1, 4, 2, 3))[None]

        def prompt_back(arr):
            return jnp.transpose(arr.reshape(layers, slots, head_dim, max_req), (0, 3, 1, 2))[None]

        return hid, dec[None], prompt_back(kp), prompt_back(vp), cache_back(k_out), cache_back(v_out)

    return jax.shard_map(local_step, mesh=mesh,
                         in_specs=(rows_spec, P('pair'), P('pair'), P(), P(), P(), P(), P(), batch_spec, cache_spec, cache_spec, rows_spec),
                         out_specs=(rows_spec, batch_spec, prompt_spec, prompt_spec, cache_spec, cache_spec),
                         check_vma=False)
```

```python
import functools
import math

import jax
import jax.numpy as jnp
from jax import lax
from jax.experimental import pallas as pl
from jax.experimental.pallas import tpu as pltpu
from jax.sharding import PartitionSpec as P

ROPE_BASE = 10000.0
NORM_EPS = 1e-5
BF16 = jnp.bfloat16
F32 = jnp.float32
TILE = 512
W_SLOTS = 18
CORES = 2
HALVES = 1
ANY = pl.BlockSpec(memory_space=pl.ANY)
VMEM = pl.BlockSpec(memory_space=pltpu.VMEM)
SMEM = pl.BlockSpec(memory_space=pltpu.SMEM)
MESH = pl.DeviceIdType.MESH
NT = (((1,), (1,)), ((), ()))


def rms(wide):
    return (wide * lax.rsqrt(jnp.mean(wide * wide, axis=-1, keepdims=True) + NORM_EPS)).astype(BF16)


def rope_tile(vals, cos, sin, head_dim):
    wide = vals.astype(F32)
    width = wide.shape[1]
    half = head_dim // 2
    lane = lax.broadcasted_iota(jnp.int32, wide.shape, 1)
    other = jnp.where(lax.rem(lane, head_dim) < half, pltpu.roll(wide, width - half, 1), pltpu.roll(wide, half, 1))
    reps = width // cos.shape[1]
    return (wide * jnp.concatenate([cos] * reps, axis=1) + other * jnp.concatenate([sin] * reps, axis=1)).astype(BF16)


def to_column(row, count, owner):
    n = row.shape[1]
    j = lax.broadcasted_iota(jnp.int32, (count, n), 0)
    return jnp.sum(jnp.where(lax.broadcasted_iota(jnp.int32, (count, n), 1) == owner(j), row.astype(F32), 0.0), axis=-1, keepdims=True)


def mega_kernel(cfg, req_ref, clen_ref, x_ref, y_ref, kc_ref, vc_ref, wq_ref, wo_ref, wg_ref, wu_ref, wd_ref,
                hid_ref, dec_ref, inst_ref, knv_ref,
                wbuf, hin, h_ref, norm_ref, acc, xch, qkv, kvwin, dsend, rdec, cback, ctx, isend, kbuf, vbuf, act_ref, gu, mask_ref, cos_ref, sin_ref, cosd_ref, sind_ref, len_ref,
                wsem, insem, csem, xsend, xrecv, kvs, kvr, kfs, dss, dsr, cbs, cbr, i1s, i1r, i2s, i2r, i3s, i3r, ilo, fhs, fhr, fds, fdr, hws, dws, flo):
    side, tp, layers, head_dim, rep, slots = cfg
    s_me = lax.axis_index('side')
    t_me = lax.axis_index('tp')
    core = lax.rem(s_me, CORES)
    col = s_me // CORES
    chip = col * tp + t_me
    chips = side // CORES * tp
    partner = s_me + 1 - 2 * core
    model = h_ref.shape[1]
    rows = h_ref.shape[0]
    p_rows = mask_ref.shape[0]
    d_rows = (rows - p_rows) // CORES
    half_p = p_rows // 2
    window = kvwin.shape[1]
    q_loc = ctx.shape[2]
    group_w = rep * head_dim
    heads = q_loc // group_w
    kv_loc = heads * head_dim
    q_all = wo_ref.shape[1]
    kv_all = (wq_ref.shape[2] - q_all) // 2
    ff_loc = wg_ref.shape[2] // CORES
    n_ff = ff_loc // TILE
    n_q = q_loc // TILE
    n_o = model * q_loc // (TILE * model)
    n_deep = ff_loc // model
    n_dn = model // TILE
    base_o = 1 + n_q
    base_g = base_o + n_o
    base_d = base_g + 2 * n_ff
    n_w = base_d + n_dn * n_deep

    def rc(src, dst, ssem, rsem, s_dev, t_dev):
        return pltpu.make_async_remote_copy(src_ref=src, dst_ref=dst, send_sem=ssem, recv_sem=rsem,
                                            device_id={'side': s_dev, 'tp': t_dev}, device_id_type=MESH)

    def at(base, size, unit):
        return pl.ds(pl.multiple_of(base, unit), size)

    def w_copies(idx):
        layer, pos = divmod(idx, n_w)
        slot = idx % W_SLOTS
        dst = wbuf.at[slot]
        if pos == 0:
            return [pltpu.make_async_copy(wq_ref.at[layer, :, at(q_all + core * kv_loc, kv_loc, 128)], dst.at[:, pl.ds(0, kv_loc)], wsem.at[slot, 0]),
                    pltpu.make_async_copy(wq_ref.at[layer, :, at(q_all + kv_all + core * kv_loc, kv_loc, 128)], dst.at[:, pl.ds(kv_loc, kv_loc)], wsem.at[slot, 1])]
        if pos < base_o:
            return [pltpu.make_async_copy(wq_ref.at[layer, :, at(core * q_loc + (pos - 1) * TILE, TILE, TILE)], dst, wsem.at[slot, 0])]
        if pos < base_g:
            pos -= base_o
            return [pltpu.make_async_copy(wo_ref.at[layer, at(core * q_loc, q_loc, q_loc), pl.ds((2 * pos + part) * TILE, TILE)], dst.at[pl.ds(part * q_loc, q_loc), :], wsem.at[slot, part]) for part in range(2)]
        if pos < base_d:
            pos -= base_g
            src = (wg_ref, wu_ref)[pos % 2]
            return [pltpu.make_async_copy(src.at[layer, :, at(core * ff_loc + (pos // 2) * TILE, TILE, TILE)], dst, wsem.at[slot, 0])]
        pos -= base_d
        return [pltpu.make_async_copy(wd_ref.at[layer, at(core * ff_loc + pos % n_deep * model, model, model), pl.ds(pos // n_deep * TILE, TILE)], dst, wsem.at[slot, 0])]

    def start_all(copies):
        for one in copies:
            one.start()

    def wait_all(copies):
        for one in copies:
            one.wait()

    def w_next(idx):
        if idx + W_SLOTS < layers * n_w:
            start_all(w_copies(idx + W_SLOTS))

    def cache_copies(layer):
        return [pltpu.make_async_copy(kc_ref.at[layer], kbuf, csem.at[0]), pltpu.make_async_copy(vc_ref.at[layer], vbuf, csem.at[1])]

    x_mine = core == t_me // (tp // CORES)
    x_src = x_ref.at[at(lax.rem(t_me, tp // CORES) * p_rows, p_rows, p_rows), :]
    x_dst = hin.at[pl.ds(0, p_rows), :]
    y_src = y_ref.at[at(t_me * d_rows, d_rows, d_rows), :]
    y_dst = hin.at[at(p_rows + core * d_rows, d_rows, d_rows), :]
    x_local = pltpu.make_async_copy(x_src, x_dst, insem.at[0])
    y_local = pltpu.make_async_copy(y_src, y_dst, insem.at[1])
    x_far = rc(x_dst, x_dst, insem.at[2], insem.at[3], partner, t_me)
    y_far = rc(y_dst, y_dst, insem.at[4], insem.at[5], partner, t_me)

    @pl.when(x_mine)
    def _():
        x_local.start()

    y_local.start()
    start_all(w_copies(0))

    barrier = pltpu.get_barrier_semaphore()
    for ds in range(side):
        for dt in range(tp):
            if ds or dt:
                pl.semaphore_signal(barrier, inc=1, device_id={'side': lax.rem(s_me + ds, side), 'tp': lax.rem(t_me + dt, tp)}, device_id_type=MESH)

    for idx in range(1, W_SLOTS):
        start_all(w_copies(idx))
        if idx == 2:
            start_all(cache_copies(0))

    for layer in range(layers):
        for dist in range(1, window // p_rows):
            @pl.when(chip < dist)
            def _():
                hi = window - p_rows * dist
                kvwin[layer, hi - p_rows:hi, :] = jnp.zeros((p_rows, kvwin.shape[2]), BF16)

    gu[...] = jnp.zeros_like(gu)

    lane = lax.broadcasted_iota(jnp.int32, (p_rows, 2 * head_dim), 1)
    freq = jnp.exp((lane & (head_dim // 2 - 1)).astype(F32) * (-math.log(ROPE_BASE) / (head_dim // 2)))
    sign = jnp.where((lane & (head_dim - 1)) < head_dim // 2, -1.0, 1.0)
    q_row = chip * p_rows + lax.broadcasted_iota(jnp.int32, (p_rows, 2 * head_dim), 0)
    seg = jnp.zeros_like(q_row)
    end = req_ref[0] * 0
    for req in range(side):
        end = end + req_ref[req]
        seg = seg + jnp.where(q_row >= end, req_ref[req], 0)
    angles = (q_row - seg).astype(F32) * freq
    cos_ref[...] = jnp.cos(angles)
    sin_ref[...] = jnp.sin(angles) * sign
    dec_pos = to_column(clen_ref[...], tp * CORES * d_rows, lambda j: (j // (CORES * d_rows)) * d_rows + (j & (d_rows - 1)))
    angles = dec_pos * freq
    cosd_ref[...] = jnp.cos(angles)
    sind_ref[...] = jnp.sin(angles) * sign
    len_ref[...] = to_column(clen_ref[...], tp * CORES * rep * d_rows, lambda j: (j // (CORES * rep * d_rows)) * d_rows + (j & (d_rows - 1))).astype(jnp.int32)
    for piece in range(window // (2 * head_dim)):
        key_row = (chip + 1) * p_rows - window + piece * 2 * head_dim + lane
        mask_ref[:, piece * 2 * head_dim:(piece + 1) * 2 * head_dim] = jnp.where((key_row <= q_row) & (key_row >= seg), 1.0, 0.0)

    pl.semaphore_wait(barrier, side * tp - 1)

    y_local.wait()
    y_far.start()

    @pl.when(x_mine)
    def _():
        x_local.wait()
        x_far.start()

    @pl.when(jnp.logical_not(x_mine))
    def _():
        x_far.wait_recv()

    y_far.wait_recv()
    h_ref[...] = hin[...].astype(F32)

    diag = (lax.broadcasted_iota(jnp.int32, (d_rows, d_rows * head_dim), 1) // head_dim) == lax.broadcasted_iota(jnp.int32, (d_rows, d_rows * head_dim), 0)
    scale = head_dim ** -0.5
    n_peer = tp * CORES

    def exchange(idx, grp):
        sl = at(grp * TILE, TILE, TILE)
        return rc(acc.at[:, sl], xch.at[idx, :, sl], xsend.at[idx, grp], xrecv.at[idx, grp], partner, t_me)

    def settle(idx, grp):
        exchange(idx, grp).wait()
        sl = at(grp * TILE, TILE, TILE)
        h_ref[:, sl] = (h_ref[:, sl] + (acc[:, sl] + xch[idx, :, sl]).astype(BF16).astype(F32)).astype(BF16).astype(F32)

    half_t = tp // CORES
    own_hid = core == t_me // half_t
    piece_me = lax.rem(t_me, half_t) * CORES + core
    n_groups = model // TILE

    def group(ref, base, size, unit, grp):
        return ref.at[at(base, size, unit), at(grp * TILE, TILE, TILE)]

    def hid_src(grp):
        return group(hin, core * half_p, half_p, half_p, grp)

    def hid_dst(grp):
        return group(hid_ref, lax.rem(t_me, half_t) * p_rows + core * half_p, half_p, half_p, grp)

    def hid_local(grp):
        return pltpu.make_async_copy(hid_src(grp), hid_dst(grp), flo.at[0, grp])

    def hid_far(grp, dt):
        return rc(hid_src(grp), hid_dst(grp), fhs.at[grp, dt], fhr.at[grp, piece_me], col * CORES + t_me // half_t, lax.rem(t_me + dt, tp))

    def dec_src(grp):
        return group(hin, p_rows + core * d_rows, d_rows, d_rows, grp)

    def dec_dst(grp):
        return group(dec_ref, t_me * d_rows, d_rows, d_rows, grp)

    def dec_local(grp):
        return pltpu.make_async_copy(dec_src(grp), dec_dst(grp), flo.at[1, grp])

    def dec_far(grp, dt):
        return rc(dec_src(grp), dec_dst(grp), fds.at[grp, dt], fdr.at[grp, dt], s_me, lax.rem(t_me + dt, tp))

    near = (1, tp - 1)

    def send_group(grp):
        sl = at(grp * TILE, TILE, TILE)
        hin[:, sl] = h_ref[:, sl].astype(BF16)
        for dt in near:
            hid_far(grp, dt).start()
            dec_far(grp, dt).start()

        @pl.when(own_hid)
        def _():
            hid_local(grp).start()

        @pl.when(jnp.logical_not(own_hid))
        def _():
            hid_far(grp, 0).start()

        dec_local(grp).start()

    partners = []
    crossed = []
    for layer in range(layers):
        w_base = layer * n_w
        norm_ref[...] = rms(h_ref[...])
        cos = cos_ref[...]
        sin = sin_ref[...]

        wait_all(w_copies(w_base))
        out = jnp.dot(norm_ref[...], wbuf[(w_base) % W_SLOTS], preferred_element_type=F32).astype(BF16)
        w_next(w_base)
        qkv[:, q_loc:] = out
        kvwin[layer, window - p_rows:, 0:kv_loc] = rope_tile(out[:p_rows, :kv_loc], cos, sin, head_dim)
        kvwin[layer, window - p_rows:, kv_loc:] = out[:p_rows, kv_loc:]

        def block(base, part):
            return kvwin.at[layer, at(base, p_rows, p_rows), pl.ds(part * kv_loc, kv_loc)]

        def halo(dist, part):
            target = chip + dist
            return rc(block(window - p_rows, part), block(window - p_rows * (dist + 1), part), kvs.at[layer, dist - 1, part], kvr.at[layer, dist - 1, part],
                      CORES * (target // tp) + core, lax.rem(target, tp))

        def goes(dist):
            return col + 1 < side // CORES if dist == tp else t_me + dist < tp

        def hand_on(place, part):
            dist = tp + place - t_me
            return rc(block(0, part), block(window - p_rows * (dist + 1), part), kfs.at[layer, place, part], kvr.at[layer, dist - 1, part], s_me, place)

        def hands_on(place):
            return (col > 0) & (place < t_me)

        for dist in (tp, 1):
            @pl.when(goes(dist))
            def _():
                for part in range(2):
                    halo(dist, part).start()

        for tile in range(n_q):
            idx = w_base + 1 + tile
            wait_all(w_copies(idx))
            out = jnp.dot(norm_ref[...], wbuf[idx % W_SLOTS], preferred_element_type=F32).astype(BF16)
            w_next(idx)
            sl = slice(tile * TILE, (tile + 1) * TILE)
            qkv[:p_rows, sl] = rope_tile(out[:p_rows], cos, sin, head_dim)
            qkv[p_rows:, sl] = out[p_rows:]

        for sub in range(CORES):
            for head in range(heads):
                r0 = p_rows + sub * d_rows
                kk = qkv[r0:r0 + d_rows, q_loc + head * head_dim:q_loc + (head + 1) * head_dim]
                vv = qkv[r0:r0 + d_rows, q_loc + kv_loc + head * head_dim:q_loc + kv_loc + (head + 1) * head_dim]
                dsend[layer, sub, head, :, 0:group_w] = qkv[r0:r0 + d_rows, head * group_w:(head + 1) * group_w]
                dsend[layer, sub, head, :, group_w:] = jnp.concatenate([kk, vv], axis=1)

        def forward(dt, dc):
            s2 = lax.rem(core + dc, CORES)
            t2 = lax.rem(t_me + dt, tp)
            return rc(dsend.at[layer, s2, t2], rdec.at[layer, t_me, core], dss.at[layer, dt * CORES + dc], dsr.at[layer, dt * CORES + dc], col * CORES + s2, t2)

        peers = [(dt, dc) for dt in range(tp) for dc in range(CORES) if dt or dc]
        for dt, dc in peers:
            forward(dt, dc).start()
        rdec[layer, t_me, core] = dsend[layer, core, t_me]
        for dist in range(2, tp):
            @pl.when(goes(dist))
            def _():
                for part in range(2):
                    halo(dist, part).start()

        for part in range(2):
            @pl.when(col > 0)
            def _():
                halo(tp, part).wait_recv()

            for place in range(tp - 1):
                @pl.when(hands_on(place))
                def _():
                    hand_on(place, part).start()

        def backward(dt, dc):
            t2 = lax.rem(t_me + tp - dt, tp)
            c2 = lax.rem(core + dc, CORES)
            dst = ctx.at[layer, at(p_rows + core * d_rows, d_rows, d_rows), at(t_me * group_w, group_w, group_w)]
            return rc(cback.at[layer, t2 * CORES + c2], dst, cbs.at[layer, dt * CORES + dc], cbr.at[layer, dt * CORES + dc], col * CORES + c2, t2)

        wait_all(cache_copies(layer))
        for dt, dc in peers:
            forward(dt, dc).wait_recv()
        raw = jnp.concatenate([rdec[layer, p // CORES, p % CORES] for p in range(n_peer)], axis=0)
        roped = rope_tile(raw, cosd_ref[...], sind_ref[...], head_dim)
        q_wide = roped[:, :group_w].astype(F32) * scale
        k_new = roped[:, group_w:group_w + head_dim].astype(F32)
        v_new = raw[:, group_w + head_dim:].astype(F32)
        eye = jnp.where(lax.broadcasted_iota(jnp.int32, (d_rows, d_rows), 0) == lax.broadcasted_iota(jnp.int32, (d_rows, d_rows), 1), 1.0, 0.0).astype(BF16)
        both = jnp.concatenate([k_new, v_new], axis=1).astype(BF16)
        scores = []
        fresh = []
        for p in range(n_peer):
            rs = slice(p * d_rows, (p + 1) * d_rows)
            knv_ref[layer, p // CORES, p % CORES] = lax.dot_general(both[rs], eye, (((0,), (0,)), ((), ())), preferred_element_type=F32).astype(BF16)
            q_parts = [q_wide[rs, r * head_dim:(r + 1) * head_dim] for r in range(rep)]
            pairs = [jnp.concatenate([part, part], axis=1) for part in q_parts]
            lhs = jnp.concatenate([jnp.where(diag, jnp.concatenate([pair] * (d_rows // 2), axis=1), 0.0) for pair in pairs], axis=0).astype(BF16)
            y2 = p // CORES
            k_part = kbuf[y2 * d_rows:(y2 + 1) * d_rows, p % CORES].reshape(d_rows * head_dim, kbuf.shape[3])
            scores.append(jnp.dot(lhs, k_part, preferred_element_type=F32))
            fresh.append(jnp.concatenate(q_parts, axis=0) * jnp.concatenate([k_new[rs]] * rep, axis=0))
        scores = jnp.concatenate(scores, axis=0)
        s_new = jnp.sum(jnp.concatenate(fresh, axis=0), axis=-1, keepdims=True)
        where_new = len_ref[...]
        pos = lax.broadcasted_iota(jnp.int32, scores.shape, 1)
        scores = jnp.where(pos < where_new, scores, -1e30)
        scores = jnp.where(pos == where_new, s_new, scores)
        scores = jnp.exp(scores - jnp.max(scores, axis=-1, keepdims=True))
        prob = (scores * (1.0 / jnp.sum(scores, axis=-1, keepdims=True))).astype(BF16).astype(F32)
        p_new = jnp.sum(jnp.where(pos == where_new, prob, 0.0), axis=-1, keepdims=True)
        p_old = jnp.where(pos == where_new, 0.0, prob).astype(BF16)
        grp_rows = rep * d_rows
        for p in range(n_peer):
            y2 = p // CORES
            gs = slice(p * grp_rows, (p + 1) * grp_rows)
            v_part = vbuf[y2 * d_rows:(y2 + 1) * d_rows, p % CORES].reshape(d_rows * head_dim, vbuf.shape[3])
            full = lax.dot_general(p_old[gs], v_part, NT, preferred_element_type=F32)
            full = jnp.where(jnp.concatenate([diag] * rep, axis=0), full, 0.0)
            fold = full[:, 0:128]
            for piece in range(1, full.shape[1] // 128):
                fold = fold + full[:, piece * 128:(piece + 1) * 128]
            got = fold[:, :head_dim] + fold[:, head_dim:] + p_new[gs] * jnp.concatenate([v_new[p * d_rows:(p + 1) * d_rows]] * rep, axis=0)
            cback[layer, p] = jnp.concatenate([got[r * d_rows:(r + 1) * d_rows] for r in range(rep)], axis=1).astype(BF16)
        for dt, dc in peers:
            backward(dt, dc).start()
        ctx[layer, at(p_rows + core * d_rows, d_rows, d_rows), at(t_me * group_w, group_w, group_w)] = cback[layer, t_me * CORES + core]
        if layer + 1 < layers:
            start_all(cache_copies(layer + 1))

        for dist in range(1, tp):
            @pl.when(chip >= dist)
            def _():
                for part in range(2):
                    halo(dist, part).wait_recv()

        allowed = mask_ref[...] > 0.5
        for head in range(heads):
            k_head = kvwin[layer, :, head * head_dim:(head + 1) * head_dim]
            v_head = kvwin[layer, :, kv_loc + head * head_dim:kv_loc + (head + 1) * head_dim]
            q0 = head * group_w
            q_part = jnp.concatenate([qkv[:p_rows, q0 + sub * head_dim:q0 + (sub + 1) * head_dim] for sub in range(rep)], axis=0)
            q_part = (q_part.astype(F32) * scale).astype(BF16)
            scores = lax.dot_general(q_part, k_head, NT, preferred_element_type=F32).reshape(rep, p_rows, window)
            scores = jnp.where(allowed[None], scores, -1e30)
            scores = jnp.exp(scores - jnp.max(scores, axis=-1, keepdims=True))
            prob = (scores * (1.0 / jnp.sum(scores, axis=-1, keepdims=True))).astype(BF16).reshape(rep * p_rows, window)
            got = jnp.dot(prob, v_head, preferred_element_type=F32).astype(BF16)
            outs = [got[sub * p_rows:(sub + 1) * p_rows] for sub in range(rep)]
            ctx[layer, 0:p_rows, q0:q0 + group_w] = jnp.concatenate(outs, axis=1)
            isend[layer, head] = jnp.concatenate([k_head[window - p_rows:], v_head[window - p_rows:]], axis=1)

        def spread(dt):
            t2 = lax.rem(t_me + dt, tp)
            return rc(isend.at[layer, t2], inst_ref.at[layer, core, at(chip * p_rows, p_rows, p_rows), :], i1s.at[layer, dt], i1r.at[layer, dt], s_me, t2)

        def keep_own():
            return pltpu.make_async_copy(isend.at[layer, t_me], inst_ref.at[layer, core, at(chip * p_rows, p_rows, p_rows), :], ilo.at[layer])

        def across(dx, layer=layer):
            part = inst_ref.at[layer, core, at(col * tp * p_rows, tp * p_rows, tp * p_rows), :]
            return rc(part, part, i2s.at[layer, dx], i2r.at[layer, dx], lax.rem(col + dx, side // CORES) * CORES + core, t_me)

        def to_partner(layer=layer):
            return rc(inst_ref.at[layer, core], inst_ref.at[layer, core], i3s.at[layer], i3r.at[layer], partner, t_me)

        def pass_on(across=across, to_partner=to_partner):
            for dx in range(1, side // CORES):
                across(dx).wait()
            to_partner().start()

        partners.append(to_partner)
        crossed.append(pass_on)
        for dt in range(1, tp):
            spread(dt).start()
        keep_own().start()
        for dt, dc in peers:
            backward(dt, dc).wait_recv()

        for tile in range(n_o):
            idx = w_base + base_o + tile
            wait_all(w_copies(idx))
            for part in range(2):
                lo = (2 * tile + part) * TILE
                acc[:, lo:lo + TILE] = jnp.dot(ctx[layer], wbuf[idx % W_SLOTS, part * q_loc:(part + 1) * q_loc, :], preferred_element_type=F32)
                exchange(2 * layer, 2 * tile + part).start()
            w_next(idx)
        for grp in range(n_groups):
            settle(2 * layer, grp)
        norm_ref[...] = rms(h_ref[...])

        def wait_slot(slot):
            pltpu.make_async_copy(wg_ref.at[layer, :, pl.ds(0, TILE)], wbuf.at[slot], wsem.at[slot, 0]).wait()

        def silu_mul(chunk):
            act_ref[:, at(chunk * TILE, TILE, TILE)] = (jax.nn.silu(gu[0].astype(F32)) * gu[1].astype(F32)).astype(BF16)

        def gate_up(chunk, carry):
            slot_g = lax.rem(w_base + base_g + 2 * chunk, W_SLOTS)
            slot_u = lax.rem(w_base + base_g + 2 * chunk + 1, W_SLOTS)
            wait_slot(slot_g)
            wait_slot(slot_u)
            gate = jnp.dot(norm_ref[...], wbuf[slot_g], preferred_element_type=F32).astype(BF16)
            silu_mul(jnp.maximum(chunk - 1, 0))
            upper = jnp.dot(norm_ref[...], wbuf[slot_u], preferred_element_type=F32).astype(BF16)
            gu[0] = gate
            gu[1] = upper
            for which in range(n_ff):
                @pl.when(chunk == which)
                def _():
                    w_next(w_base + base_g + 2 * which)
                    w_next(w_base + base_g + 2 * which + 1)
            return carry

        lax.fori_loop(0, n_ff, gate_up, 0)
        silu_mul(n_ff - 1)
        if layer:
            crossed[layer - 1]()
        for dt in range(1, tp):
            spread(dt).wait()
        keep_own().wait()
        for dx in range(1, side // CORES):
            across(dx).start()

        last = layer + 1 == layers

        def down(tile, carry):
            total = None
            for deep in range(n_deep):
                slot = lax.rem(w_base + base_d + tile * n_deep + deep, W_SLOTS)
                wait_slot(slot)
                part = jnp.dot(act_ref[:, deep * model:(deep + 1) * model], wbuf[slot], preferred_element_type=F32)
                total = part if total is None else total + part
            acc[:, at(tile * TILE, TILE, TILE)] = total
            exchange(2 * layer + 1, tile).start()
            for which in range(n_dn):
                @pl.when(tile == which)
                def _():
                    for deep in range(n_deep):
                        w_next(w_base + base_d + which * n_deep + deep)

            @pl.when(tile > 1)
            def _():
                settle(2 * layer + 1, tile - 2)
                if last:
                    send_group(tile - 2)
            return carry

        lax.fori_loop(0, n_dn, down, 0)
        for grp in range(n_dn - 2, n_dn):
            settle(2 * layer + 1, grp)
            if last:
                send_group(grp)

        for dist in range(1, tp + 1):
            @pl.when(goes(dist))
            def _():
                for part in range(2):
                    halo(dist, part).wait_send()
        for place in range(tp - 1):
            @pl.when(hands_on(place))
            def _():
                for part in range(2):
                    hand_on(place, part).wait_send()
        for dt, dc in peers:
            forward(dt, dc).wait_send()
            backward(dt, dc).wait_send()
        if layer == 0:
            @pl.when(x_mine)
            def _():
                x_far.wait_send()

            y_far.wait_send()

    def hid_piece(grp, sub, c2):
        return hid_ref.at[pl.ds(sub * p_rows + c2 * half_p, half_p), pl.ds(grp * TILE, TILE)]

    def hid_pass(grp, sub, c2):
        return rc(hid_piece(grp, sub, c2), hid_piece(grp, sub, c2), hws.at[grp, sub * CORES + c2], fhr.at[grp, sub * CORES + c2], s_me, lax.rem(t_me + near[grp % 2], tp))

    def dec_pass(grp):
        piece = group(dec_ref, lax.rem(t_me + tp - near[grp % 2], tp) * d_rows, d_rows, d_rows, grp)
        return rc(piece, piece, dws.at[grp], fdr.at[grp, 2], s_me, lax.rem(t_me + near[grp % 2], tp))

    def origin(sub):
        return lax.rem(t_me + tp - (core * half_t + sub), tp)

    direct = [(sub, c2) for sub in range(half_t) for c2 in range(CORES)]
    for grp in range(n_groups):
        for sub, c2 in direct:
            gap = origin(sub)

            @pl.when((gap != 2) & jnp.logical_not((gap == 0) & (core == c2)))
            def _():
                hid_pass(grp, sub, c2).wait_recv()

            @pl.when(gap == near[grp % 2])
            def _():
                hid_pass(grp, sub, c2).start()

        dec_far(grp, near[grp % 2]).wait_recv()
        dec_pass(grp).start()
    crossed[-1]()
    for grp in range(n_groups):
        dec_far(grp, near[1 - grp % 2]).wait_recv()
        dec_far(grp, 2).wait_recv()
        for sub, c2 in direct:
            gap = origin(sub)

            @pl.when(gap == 2)
            def _():
                hid_pass(grp, sub, c2).wait_recv()

            @pl.when(gap == near[grp % 2])
            def _():
                hid_pass(grp, sub, c2).wait_send()

        dec_pass(grp).wait_send()
        for dt in near:
            hid_far(grp, dt).wait_send()
            dec_far(grp, dt).wait_send()

        @pl.when(own_hid)
        def _():
            hid_local(grp).wait()

        @pl.when(jnp.logical_not(own_hid))
        def _():
            hid_far(grp, 0).wait_send()

        dec_local(grp).wait()
    for handed in partners:
        handed().wait()


def finish_kernel(req_ref, dest_ref, len_ref, knv_hbm, hid_ref, dec_ref, inst_ref, k_ref, v_ref,
                  hout_ref, dout_ref, kp_out, vp_out, kout_ref, vout_ref, kv_buf, ibuf, hbuf, dbuf, knv_ref, kp_ref, vp_ref, ksem, isem, hsem):
    layers, tp, slots, wide, batch = knv_ref.shape
    head_dim = wide // 2
    t_len = kv_buf.shape[5]
    win = ibuf.shape[2]
    max_req = kp_ref.shape[2]
    s_me = lax.axis_index('side')
    total_b = tp * batch
    units = [(layer, which, half) for layer in range(layers) for half in range(HALVES) for which in range(2)]
    part_b = total_b // HALVES

    def caches(num, out):
        layer, which, half = units[num]
        rows = pl.ds(half * part_b, part_b)
        far = ((k_ref, v_ref), (kout_ref, vout_ref))[out][which].at[layer, rows]
        near = kv_buf.at[layer, which, rows]
        return pltpu.make_async_copy(near, far, ksem.at[num, 1]) if out else pltpu.make_async_copy(far, near, ksem.at[num, 0])

    cum = req_ref[0] * 0
    start = cum
    length = cum
    for req in range(req_ref.shape[0]):
        start = jnp.where(dest_ref[req] == s_me, cum, start)
        length = jnp.where(dest_ref[req] == s_me, req_ref[req], length)
        cum = cum + req_ref[req]
    blk = jnp.minimum((start // 64) * 64, inst_ref.shape[2] - win)
    grabs = [pltpu.make_async_copy(inst_ref.at[layer, :, pl.ds(pl.multiple_of(blk, 64), win), :], ibuf.at[layer], isem.at[layer]) for layer in range(layers)]
    knv_in = pltpu.make_async_copy(knv_hbm, knv_ref, hsem.at[4])
    prompt_out = [pltpu.make_async_copy(kp_ref, kp_out, hsem.at[5]), pltpu.make_async_copy(vp_ref, vp_out, hsem.at[6])]
    knv_in.start()
    for num in range(2):
        caches(num, 0).start()
    for one in grabs:
        one.start()
    h_in = [pltpu.make_async_copy(hid_ref, hbuf, hsem.at[0]), pltpu.make_async_copy(dec_ref, dbuf, hsem.at[1])]
    h_out = [pltpu.make_async_copy(hbuf, hout_ref, hsem.at[2]), pltpu.make_async_copy(dbuf, dout_ref, hsem.at[3])]
    row = blk + lax.broadcasted_iota(jnp.int32, (win, max_req), 0)
    want = lax.broadcasted_iota(jnp.int32, (win, max_req), 1)
    pick = jnp.where((row - start == want) & (want < length), 1.0, 0.0).astype(BF16)
    knv_in.wait()
    t_iota = lax.broadcasted_iota(jnp.int32, (head_dim, t_len), 1)
    for num, (layer, which, half) in enumerate(units):
        caches(num, 0).wait()
        if num + 2 < len(units):
            caches(num + 2, 0).start()
            if num == 1:
                for one in h_in:
                    one.start()
        for b in range(half * part_b, (half + 1) * part_b):
            here = t_iota == len_ref[b]
            for slot in range(slots):
                new = knv_ref[layer, b // batch, slot, which * head_dim:(which + 1) * head_dim, b % batch:b % batch + 1].astype(F32)
                kv_buf[layer, which, b, slot] = jnp.where(here, new, kv_buf[layer, which, b, slot].astype(F32)).astype(BF16)
        caches(num, 1).start()
        if num == 1:
            for lay in range(layers):
                grabs[lay].wait()
                for slot in range(slots):
                    both = lax.dot_general(ibuf[lay, slot], pick, (((0,), (0,)), ((), ())), preferred_element_type=F32).astype(BF16)
                    kp_ref[lay, slot * head_dim:(slot + 1) * head_dim, :] = both[:head_dim]
                    vp_ref[lay, slot * head_dim:(slot + 1) * head_dim, :] = both[head_dim:]
            for one in prompt_out:
                one.start()
    for one in h_in:
        one.wait()
    for one in h_out:
        one.start()
    for num in range(len(units)):
        caches(num, 1).wait()
    for one in h_out + prompt_out:
        one.wait()


def solution(mesh):
    tp = mesh.shape['tp']
    side = mesh.shape['side']
    rows_spec = P(('pair', 'side'), None)
    batch_spec = P(('pair', 'side'), None, None)
    cache_spec = P(('pair', 'side'), None, None, None, 'tp', None)
    prompt_spec = P(('pair', 'side'), None, None, 'tp', None)

    def local_step(x_loc, req_len, dest, w_qkv, w_out, w_gate, w_up, w_down, y_loc, kc_loc, vc_loc, clen_loc):
        layers = w_qkv.shape[0]
        head_dim = kc_loc.shape[-1]
        slots = kc_loc.shape[-2]
        t_len = kc_loc.shape[3]
        batch = y_loc.shape[1]
        kv_heads = slots * tp
        rep = w_out.shape[1] // head_dim // kv_heads
        model = x_loc.shape[1]
        prompt_rows = x_loc.shape[0]
        seq_len = prompt_rows * side
        max_req = 2 * prompt_rows - prompt_rows // 4
        p_rows = prompt_rows * CORES // tp
        d_rows = batch // tp
        rows = p_rows + CORES * d_rows
        q_loc = w_out.shape[1] // CORES
        kv_loc = kv_heads // CORES * head_dim
        heads = kv_heads // CORES
        window = -(-(max_req - 1) // p_rows) * p_rows + p_rows
        assert window == (tp + 1) * p_rows
        group_w = rep * head_dim

        lengths = clen_loc[0]
        kc = jnp.transpose(kc_loc[0], (0, 1, 3, 4, 2))
        vc = jnp.transpose(vc_loc[0], (0, 1, 3, 4, 2))
        ff_loc = w_gate.shape[2] // CORES
        groups = model // TILE

        dma = pltpu.SemaphoreType.DMA
        n_peer = tp * CORES
        hid, dec, inst, knv = pl.pallas_call(
            functools.partial(mega_kernel, (side, tp, layers, head_dim, rep, slots)),
            out_shape=[jax.ShapeDtypeStruct((prompt_rows, model), BF16), jax.ShapeDtypeStruct((batch, model), BF16),
                       jax.ShapeDtypeStruct((layers, CORES, seq_len, 2 * head_dim), BF16),
                       jax.ShapeDtypeStruct((layers, tp, CORES, 2 * head_dim, d_rows), BF16)],
            in_specs=[SMEM, VMEM, ANY, ANY, ANY, ANY, ANY, ANY, ANY, ANY, ANY],
            out_specs=[ANY, ANY, ANY, VMEM],
            scratch_shapes=[
                pltpu.VMEM((W_SLOTS, model, TILE), BF16),
                pltpu.VMEM((rows, model), BF16),
                pltpu.VMEM((rows, model), F32),
                pltpu.VMEM((rows, model), BF16),
                pltpu.VMEM((rows, model), F32),
                pltpu.VMEM((2 * layers, rows, model), F32),
                pltpu.VMEM((rows, q_loc + 2 * kv_loc), BF16),
                pltpu.VMEM((layers, window, 2 * kv_loc), BF16),
                pltpu.VMEM((layers, CORES, heads, d_rows, group_w + 2 * head_dim), BF16),
                pltpu.VMEM((layers, tp, CORES, d_rows, group_w + 2 * head_dim), BF16),
                pltpu.VMEM((layers, n_peer, d_rows, group_w), BF16),
                pltpu.VMEM((layers, rows, q_loc), BF16),
                pltpu.VMEM((layers, heads, p_rows, 2 * head_dim), BF16),
                pltpu.VMEM((batch, slots, head_dim, t_len), BF16),
                pltpu.VMEM((batch, slots, head_dim, t_len), BF16),
                pltpu.VMEM((rows, ff_loc), BF16),
                pltpu.VMEM((2, rows, TILE), BF16),
                pltpu.VMEM((p_rows, window), F32),
                pltpu.VMEM((p_rows, 2 * head_dim), F32), pltpu.VMEM((p_rows, 2 * head_dim), F32),
                pltpu.VMEM((n_peer * d_rows, 2 * head_dim), F32), pltpu.VMEM((n_peer * d_rows, 2 * head_dim), F32),
                pltpu.VMEM((n_peer * rep * d_rows, 1), jnp.int32),
                dma((W_SLOTS, 2)), dma((6,)), dma((2,)),
                dma((2 * layers, groups)), dma((2 * layers, groups)),
                dma((layers, tp, 2)), dma((layers, tp, 2)), dma((layers, tp, 2)),
                dma((layers, n_peer)), dma((layers, n_peer)),
                dma((layers, n_peer)), dma((layers, n_peer)),
                dma((layers, tp)), dma((layers, tp)), dma((layers, side // CORES)), dma((layers, side // CORES)), dma((layers,)), dma((layers,)), dma((layers,)),
                dma((groups, tp)), dma((groups, tp)), dma((groups, tp)), dma((groups, tp)), dma((groups, tp)), dma((groups,)), dma((2, groups)),
            ],
            compiler_params=pltpu.CompilerParams(collective_id=0, has_side_effects=True, vmem_limit_bytes=67043328),
            name="mega",
        )(req_len, clen_loc, x_loc, y_loc[0], kc, vc, w_qkv, w_out, w_gate, w_up, w_down)

        win = 512
        hid, dec, kp, vp, k_out, v_out = pl.pallas_call(
            finish_kernel,
            out_shape=[jax.ShapeDtypeStruct(hid.shape, BF16), jax.ShapeDtypeStruct(dec.shape, BF16)]
            + [jax.ShapeDtypeStruct((layers, slots * head_dim, max_req), BF16)] * 2 + [jax.ShapeDtypeStruct(kc.shape, BF16)] * 2,
            in_specs=[SMEM, SMEM, SMEM, ANY, ANY, ANY, ANY, ANY, ANY],
            out_specs=[ANY] * 6,
            scratch_shapes=[
                pltpu.VMEM((layers, 2, batch, slots, head_dim, t_len), BF16),
                pltpu.VMEM((layers, slots, win, 2 * head_dim), BF16),
                pltpu.VMEM(hid.shape, BF16), pltpu.VMEM(dec.shape, BF16), pltpu.VMEM(knv.shape, BF16),
                pltpu.VMEM((layers, slots * head_dim, max_req), BF16), pltpu.VMEM((layers, slots * head_dim, max_req), BF16),
                dma((2 * layers * HALVES, 2)), dma((layers,)), dma((7,)),
            ],
            compiler_params=pltpu.CompilerParams(vmem_limit_bytes=67043328),
            name="finish",
        )(req_len, dest, lengths, knv, hid, dec, inst, kc, vc)

        def cache_back(arr):
            return jnp.transpose(arr, (0, 1, 4, 2, 3))[None]

        def prompt_back(arr):
            return jnp.transpose(arr.reshape(layers, slots, head_dim, max_req), (0, 3, 1, 2))[None]

        return hid, dec[None], prompt_back(kp), prompt_back(vp), cache_back(k_out), cache_back(v_out)

    return jax.shard_map(local_step, mesh=mesh,
                         in_specs=(rows_spec, P('pair'), P('pair'), P(), P(), P(), P(), P(), batch_spec, cache_spec, cache_spec, rows_spec),
                         out_specs=(rows_spec, batch_spec, prompt_spec, prompt_spec, cache_spec, cache_spec),
                         check_vma=False)
```
